128 devices in a mesh: row: 8 (over z, y_hi), col: 16 (over y_lo, x, core).
Axes of the slice: x: 4, y: 4 (y_hi: 2, y_lo: 2; y = y_hi * 2 + y_lo), z: 4, core: 2. Of those that a mesh axis runs over, the one named last changes fastest.
Arguments:
- matrix: float32 [16, 1024, 8, 2048], P(None, 'row', None, 'col'), may hold values from -150 to 150
- inverse_rest: float32 [16, 1024, 7, 2048], P(None, 'row', None, 'col'), may hold values from -6 to 6
- upper_block: float32 [2, 1024, 1, 2048], P(None, 'row', None, 'col'), may hold values from -6 to 6, as said below
- lower_below: float32 [2, 1024, 7, 2048], P(None, 'row', None, 'col'), may hold values from -0.046875 to 0.046875
- lower_inverse: float32 [2, 1024, 2048], P(None, 'row', 'col'), may hold values from -1 to 1, as said below
Outputs:
- plus_rows: float32 [2, 1024, 8, 2048], P(None, 'row', None, 'col')
The draws below stay inside these ranges and needn't reach their ends.
Inputs may be any that keep to these rules, and one draw needn't show every extreme that they name: `upper_block`: upper triangular. `lower_inverse`: unit lower triangular.
All inputs are finite; a program needn't handle non-finite values.
Results may differ from the reference program's by a relative error of at most 0.000052.
Values sent between devices are 32-bit elements; how exact they have to be, the bound alone decides.
A program may use at most 192 MiB of HBM per device.

```python
import jax
import jax.numpy as jnp
from jax import lax

N = 16384
BLK = 128
W = 2048
REST = 14336
KR = 16
KC = 8
KWR = 2
KW = 1
KCR = 7
N_ROW = 8
N_COL = 16


def draw_matrix(key, part):
    row_key, col_key, base_key = jax.random.split(jax.random.fold_in(key, 17), 3)
    row_scale = jnp.exp(jax.random.uniform(row_key, (N, 1), jnp.float32, 0.0, 2.302585))
    col_scale = jnp.exp(jax.random.uniform(col_key, (1, N), jnp.float32, 0.0, 2.302585))
    values = jnp.clip(jax.random.normal(base_key, (N, N), jnp.float32), -6.0, 6.0)
    return (values * row_scale * col_scale * 0.25).reshape(KR, N // KR, KC, N // KC)


def draw_upper_block(key, part):
    base_key = jax.random.fold_in(key, 23)
    values = jnp.clip(jax.random.normal(base_key, (W, W), jnp.float32), -6.0, 6.0)
    return jnp.triu(values).reshape(KWR, W // KWR, KW, W // KW)


def draw_lower_inverse(key, part):
    base_key = jax.random.fold_in(key, 29)
    values = jnp.clip(jax.random.normal(base_key, (W, W), jnp.float32), -6.0, 6.0) * (0.5 / jnp.sqrt(W * 1.0))
    unit_lower = jnp.eye(W, dtype=jnp.float32) + jnp.tril(values, -1)
    return unit_lower.reshape(KWR, W // KWR, W)


def block_levels(own_key, extent, cuts, smallest, largest):
    loudness = 1.0
    for axis_at, blocks in cuts:
        draws = jax.random.uniform(jax.random.fold_in(jax.random.fold_in(own_key, 6), axis_at), (blocks,), jnp.float32, smallest / len(cuts), largest / len(cuts))
        loudness = loudness * jnp.repeat(jnp.exp(draws), extent[axis_at] // blocks).reshape((-1,) + (1,) * (len(extent) - 1 - axis_at))
    return loudness


def noise(key, dims, spread, reach, pieces=(), held_as=jnp.bfloat16):
    values = spread * jax.random.normal(key, dims, jnp.float32)
    if pieces:
        values = values * block_levels(key, dims, pieces, -0.22, 0.18)
    return jnp.clip(values, -reach, reach).astype(held_as)


def setup_inputs(seed: int = 0) -> dict:
    seeds = jax.random.split(jax.random.key(seed), 6)
    matrix = draw_matrix(jax.random.fold_in(seeds[5], 71), 0)
    inverse_rest = noise(seeds[1], (KR, N_ROW * BLK, KCR, N_COL * BLK), 1.0, 6.0, ((1, 8), (3, 16)), jnp.float32)
    upper_block = draw_upper_block(jax.random.fold_in(seeds[5], 71), 0)
    lower_below = noise(seeds[3], (KWR, N_ROW * BLK, KCR, N_COL * BLK), REST ** -0.5, 0.046875, ((1, 8), (3, 16)), jnp.float32)
    lower_inverse = draw_lower_inverse(jax.random.fold_in(seeds[5], 71), 0)
    return {"matrix": matrix, "inverse_rest": inverse_rest, "upper_block": upper_block, "lower_below": lower_below, "lower_inverse": lower_inverse}


def reference(matrix, inverse_rest, upper_block, lower_below, lower_inverse):
    whole_matrix = matrix.reshape(N, N)
    rest_inverse = inverse_rest.reshape(N, N - W)
    upper_part = upper_block.reshape(W, W)
    below_part = lower_below.reshape(W, N - W)
    factor_part = lower_inverse.reshape(W, W)
    correction = jnp.dot(rest_inverse, below_part.T, precision=lax.Precision.HIGHEST, preferred_element_type=jnp.float32)
    update_panel = jnp.concatenate([upper_part, jnp.zeros((N - W, W), jnp.float32)], axis=0) - correction
    inverse_panel = jnp.dot(update_panel, factor_part, precision=lax.Precision.HIGHEST, preferred_element_type=jnp.float32)
    matrix_norm = jnp.sum(whole_matrix * whole_matrix)
    inverse_norm = jnp.sum(rest_inverse * rest_inverse) + jnp.sum(inverse_panel * inverse_panel)
    balance = jnp.sqrt(jnp.sqrt(inverse_norm / matrix_norm))
    plus_rows = 0.5 * (balance * whole_matrix[:W] + inverse_panel.T / balance)
    return plus_rows.reshape(KWR, W // KWR, KC, N // KC)
```

```python
import jax
import jax.numpy as jnp
from jax import lax
from jax.experimental import pallas as pl
from jax.experimental.pallas import tpu as pltpu
from jax.sharding import Mesh
from jax.sharding import PartitionSpec as P

ROW = ("row_0", "row_1")
COL = ("col_0", "col_1", "col_2")
MESH = pl.DeviceIdType.MESH
F32 = jnp.float32
BF16 = jnp.bfloat16
ANY = pl.ANY

S_BELOW = 0
S_FWD = 16
S_PAIR = 18
S_A = 26
S_B = 42
S_Y = 58
S_L = 66
S_OUT = 77
S_M1 = 78
S_M2 = 86
S_SUM = 94
N_SEM = 104


def split(value):
    hi = value.astype(BF16)
    lo = (value - hi.astype(F32)).astype(BF16)
    return hi, lo


def dot_t(a, b):
    return lax.dot_general(a, b, (((1,), (1,)), ((), ())), preferred_element_type=F32)


def dot_n(a, b):
    return lax.dot_general(a, b, (((1,), (0,)), ((), ())), preferred_element_type=F32)


def rows_at(block, count):
    return pl.ds(pl.multiple_of(block * 128, 128), count * 128)


def kernel(
    mat, rest, up, below, linv, out,
    ball, yfwd, rcat, bcat, part, pair, rec_a, rec_b, rec_y, xy, xs, lall, acc, acc_in,
    m1, m2, top, mstage, rstage, ublk, lstage, sums, sums_in,
    in_sem, r_sem, m_sem, send, recv,
):
    z = lax.axis_index("row_0")
    yh = lax.axis_index("row_1")
    yl = lax.axis_index("col_0")
    x = lax.axis_index("col_1")
    h = lax.axis_index("col_2")
    me_r = z * 2 + yh

    def dev(dz=0, dyh=0, dyl=0, dx=0, dh=0):
        return ((z + dz) % 4, (yh + dyh) % 2, (yl + dyl) % 2, (x + dx) % 4, (h + dh) % 2)

    y = yh * 2 + yl

    def dev_y(dy):
        there = (y + dy) % 4
        return (z, there // 2, there % 2, x, h)

    def copy(src, dst, index, device):
        return pltpu.make_async_remote_copy(
            src_ref=src, dst_ref=dst, send_sem=send.at[index], recv_sem=recv.at[index],
            device_id=device, device_id_type=MESH,
        )

    partner = dev(dh=1)
    zp, zm = dev(dz=1), dev(dz=3)
    xp, xm = dev(dx=1), dev(dx=3)
    yp, ym = dev_y(1), dev_y(3)
    ypair = dev(dyl=1)

    load_below = [pltpu.make_async_copy(below.at[k], ball.at[me_r, k], in_sem.at[k]) for k in range(2)]
    load_l = pltpu.make_async_copy(linv, lstage, in_sem.at[2])
    load_u = pltpu.make_async_copy(up, ublk, in_sem.at[3])
    load_top = pltpu.make_async_copy(mat.at[pl.ds(0, 2)], top, in_sem.at[4])
    for load in (*load_below, load_l, load_u):
        load.start()

    def load_r(p):
        return pltpu.make_async_copy(rest.at[p], rstage.at[p % 2], r_sem.at[p % 2])

    def load_m(p):
        return pltpu.make_async_copy(mat.at[p], mstage.at[p % 2], m_sem.at[p % 2])

    load_r(0).start()
    load_r(1).start()
    load_top.start()

    barrier = pltpu.get_barrier_semaphore()
    friends = [dev(dz=dz, dyh=dyh) for dz in range(4) for dyh in range(2) if (dz, dyh) != (0, 0)]
    friends += [dev(dx=dx, dh=dh) for dx in range(4) for dh in range(2) if (dx, dh) != (0, 0)]
    friends += [yp, ym]
    for friend in friends:
        pl.semaphore_signal(barrier, inc=1, device_id=friend, device_id_type=MESH)
    pl.semaphore_wait(barrier, len(friends))

    def below_copy(source, half, step, device):
        ref = ball.at[source, half]
        return copy(ref, ref, S_BELOW + 2 * step + half, device)

    for load in load_below:
        load.wait()
    below_copy(me_r, 0, 1, zp).start()
    below_copy(me_r, 1, 2, zm).start()
    copy(ball.at[me_r, 0], yfwd.at[0], S_FWD, yp).start()
    copy(ball.at[me_r, 1], yfwd.at[1], S_FWD + 1, ym).start()
    below_copy(me_r, 1, 1, zp).start()
    below_copy(me_r, 0, 2, zm).start()

    my_pair = lall.at[yl, yh, z, x]
    load_l.wait()
    swap_l = copy(lstage.at[1 - h], lall.at[yl, yh, z, x, :, pl.ds(pl.multiple_of(h * 128, 128), 128)], S_L, partner)
    swap_l.start()
    for core in range(2):
        @pl.when(h == core)
        def _():
            lall[yl, yh, z, x, :, core * 128:(core + 1) * 128] = lstage[core]

    mine_l = jnp.logical_or(h == 1, yl == 0)
    beside_l = jnp.logical_or(h == 1, yl == 1)

    def spread_l(ref, base, which):
        for j in range(1, 4):
            yield copy(ref, ref, base + j - 1, dev(dx=j) if which == "x" else dev(dz=j))

    def l_copy(index, dy):
        ref = lall.at[yl, yh]
        return copy(ref, ref, S_L + index, dev_y(dy))

    def l_forward(index, from_dy, to_dy, first):
        there = (y + from_dy) % 4
        ref = lall.at[there % 2, there // 2, pl.ds(first, 2)]
        return copy(ref, ref, S_L + index, dev_y(to_dy))

    sums[...] = jnp.zeros(sums.shape, F32)

    def take_r(p, carry):
        load_r(p).wait()
        base = ((p // 4) * 4 + (p % 2) * 2 + (p // 2) % 2) * 128
        total = jnp.zeros((8, 128), F32)
        for q in range(7):
            value = rstage[p % 2, q]
            total += jnp.sum((value * value).reshape(16, 8, 128), axis=0)
            hi, lo = split(value)
            where = pl.ds(pl.multiple_of(base, 128), 128)
            rcat[where, q * 128:(q + 1) * 128] = hi
            rcat[where, (7 + q) * 128:(8 + q) * 128] = lo
        sums[0, 1] += total

        @pl.when(p + 2 < 16)
        def _():
            load_r(p + 2).start()

        return carry

    lax.fori_loop(0, 16, take_r, 0)
    load_u.wait()

    def source(step):
        j = step % 4
        dz = jnp.where(j == 1, 3, jnp.where(j == 2, 1, jnp.where(j == 3, 2, 0)))
        return (z + dz) % 4, (yh + step // 4) % 2

    def pair_copy(s):
        return copy(part.at[s % 4, 1 - h], pair.at[s], S_PAIR + s, partner)

    def a_copy(s, side):
        far = (x + 2) % 4
        src = part.at[s % 4, h, rows_at(far * 4 + 2 * side, 2)]
        return copy(src, rec_a.at[s, side], S_A + 2 * s + side, xp if side == 0 else xm)

    def b_copy(s, side):
        near = (x + (1 if side == 0 else 3)) % 4
        src = part.at[s % 4, h, rows_at(near * 4, 4)]
        return copy(src, rec_b.at[s, side], S_B + 2 * s + side, xp if side == 0 else xm)

    def y_copy(s):
        return copy(xy.at[s, rows_at((1 - yl) * 2, 2)], rec_y.at[s], S_Y + s, ypair)

    def step_body(t, carry):
        @pl.when(t < 8)
        def _():
            load_m(2 * t).start()
            load_m(2 * t + 1).start()

        @pl.when(jnp.logical_and(t >= 1, t < 9))
        def _():
            s = t - 1
            pair_copy(s).wait_recv()

            def add(i, carry):
                where = rows_at(((i + 4 * (x + 2)) % 16), 1)
                part[s % 4, h, where] += pair[s, where]
                return carry

            lax.fori_loop(0, 4, add, 0)
            a_copy(s, 0).start()
            a_copy(s, 1).start()
            lax.fori_loop(4, 16, add, 0)

        @pl.when(jnp.logical_and(t >= 2, t < 10))
        def _():
            s = t - 2
            for side in range(2):
                a_copy(s, side).wait_recv()
                near = (x + (1 if side == 0 else 3)) % 4
                where = rows_at(near * 4 + 2 * side, 2)
                part[s % 4, h, where] += rec_a[s, side]
                b_copy(s, side).start()

        @pl.when(t == 1)
        def _():
            below_copy(source(1)[0] * 2 + source(1)[1], 0, 1, zp).wait_recv()
            below_copy(source(1)[0] * 2 + source(1)[1], 0, 3, zp).start()
            below_copy(source(2)[0] * 2 + source(2)[1], 1, 2, zm).wait_recv()
            below_copy(source(2)[0] * 2 + source(2)[1], 1, 3, zm).start()
            copy(yfwd.at[0], yfwd.at[0], S_FWD, yp).wait_recv()
            copy(yfwd.at[1], yfwd.at[1], S_FWD + 1, ym).wait_recv()
            back = (y + 3) % 4
            copy(yfwd.at[0], ball.at[z * 2 + back // 2, 0], S_BELOW + 8, yp).start()
            ahead = (y + 1) % 4
            copy(yfwd.at[1], ball.at[z * 2 + ahead // 2, 1], S_BELOW + 9, ym).start()
            swap_l.wait_recv()

            @pl.when(mine_l)
            def _():
                for c in spread_l(my_pair, S_L + 1, "x"):
                    c.start()

        @pl.when(t == 2)
        def _():
            r4 = source(4)[0] * 2 + source(4)[1]
            below_copy(r4, 0, 4, zp).wait_recv()
            below_copy(r4, 1, 4, zp).wait_recv()
            below_copy(r4, 0, 5, zp).start()
            below_copy(r4, 1, 6, zm).start()
            below_copy(r4, 1, 5, zp).start()
            below_copy(r4, 0, 6, zm).start()

            @pl.when(mine_l)
            def _():
                for c in spread_l(my_pair, S_L + 1, "x"):
                    c.wait_recv()
                for c in spread_l(lall.at[yl, yh, z], S_L + 4, "z"):
                    c.start()

        @pl.when(t == 3)
        def _():
            @pl.when(mine_l)
            def _():
                for c in spread_l(lall.at[yl, yh, z], S_L + 4, "z"):
                    c.wait_recv()
                l_copy(7, 1).start()
                l_copy(8, 3).start()

        @pl.when(t == 5)
        def _():
            r5 = source(5)[0] * 2 + source(5)[1]
            below_copy(r5, 0, 5, zp).wait_recv()
            below_copy(r5, 0, 7, zp).start()
            r6 = source(6)[0] * 2 + source(6)[1]
            below_copy(r6, 1, 6, zm).wait_recv()
            below_copy(r6, 1, 7, zm).start()

        @pl.when(t == 8)
        def _():
            @pl.when(beside_l)
            def _():
                l_copy(7, 1).wait_recv()
                l_forward(9, 3, 1, 0).start()
                l_copy(8, 3).wait_recv()
                l_forward(10, 1, 3, 2).start()

        @pl.when(t < 8)
        def _():
            zs, ys = source(t)
            r = zs * 2 + ys
            seen0 = jnp.logical_or(jnp.logical_or(t == 0, t == 1), jnp.logical_or(t == 4, t == 5))
            seen1 = jnp.logical_or(jnp.logical_or(t == 0, t == 2), jnp.logical_or(t == 4, t == 6))

            @pl.when(jnp.logical_not(seen0))
            def _():
                below_copy(r, 0, t, zp).wait_recv()

            @pl.when(jnp.logical_not(seen1))
            def _():
                below_copy(r, 1, t, zp).wait_recv()

            for k in range(2):
                for q in range(7):
                    hi, lo = split(ball[r, k, q])
                    where = slice(k * 128, (k + 1) * 128)
                    bcat[where, q * 128:(q + 1) * 128] = hi
                    bcat[where, (7 + q) * 128:(8 + q) * 128] = hi
                    bcat[where, (14 + q) * 128:(15 + q) * 128] = lo

            def tile(i, carry):
                where = rows_at(2 * i, 2)
                value = dot_t(rcat[where, 0:1792], bcat[:, 0:1792]) + dot_t(rcat[where, 0:896], bcat[:, 1792:2688])
                part[t % 4, 0, where] = value[:, :128]
                part[t % 4, 1, where] = value[:, 128:]
                return carry

            lax.fori_loop(0, 8, tile, 0)

            @pl.when((yl * 8 + x * 2 + h) % 8 == r)
            def _():
                for k in range(2):
                    part[t % 4, yl, k * 256:k * 256 + 128] -= ublk[k]

            pair_copy(t).start()

            for slot in range(2):
                load_m(2 * t + slot).wait()
                value = mstage[slot]
                sums[0, 0] += jnp.sum((value * value).reshape(128, 8, 128), axis=0)

        @pl.when(jnp.logical_and(t >= 3, t < 11))
        def _():
            s = t - 3
            b_copy(s, 0).wait_recv()
            b_copy(s, 1).wait_recv()

            def add(i, carry):
                where = rows_at(i, 1)
                xy[s, where] = part[s % 4, h, rows_at(x * 4 + i, 1)] + rec_b[s, 0, where] + rec_b[s, 1, where]
                return carry

            lax.fori_loop(0, 4, add, 0)
            y_copy(s).start()
            pair_copy(s).wait_send()
            for side in range(2):
                a_copy(s, side).wait_send()
                b_copy(s, side).wait_send()

        @pl.when(t >= 4)
        def _():
            s = t - 4
            y_copy(s).wait_recv()
            value = xy[s, rows_at(yl * 2, 2)] + rec_y[s]
            hi, lo = split(value)
            xs[s, :, 0:128] = hi
            xs[s, :, 128:256] = lo

        return carry

    lax.fori_loop(0, 12, step_body, 0)

    @pl.when(mine_l)
    def _():
        l_forward(9, 3, 1, 0).wait_recv()
        l_forward(10, 1, 3, 2).wait_recv()

    n_pairs = 4 + 4 * h

    def clear(i, carry):
        acc[i] = jnp.zeros((256, 256), F32)
        return carry

    lax.fori_loop(0, n_pairs, clear, 0)

    def product(s, carry):
        zs, ys = source(s)

        def one(i, carry):
            hi, lo = split(lall[i // 4, ys, zs, i % 4])
            acc[i] += dot_n(xs[s], jnp.concatenate([hi, hi], axis=0)) + dot_n(xs[s, :, 0:128], lo)
            return carry

        lax.fori_loop(0, n_pairs, one, 0)
        return carry

    lax.fori_loop(0, 8, product, 0)

    out_copy = copy(acc.at[pl.ds(0, 4)], acc_in, S_OUT, partner)

    @pl.when(h == 1)
    def _():
        out_copy.start()

    @pl.when(h == 0)
    def _():
        out_copy.wait_recv()

        def add(i, carry):
            acc[i] += acc_in[i]
            return carry

        lax.fori_loop(0, 4, add, 0)

    def squares(i, carry):
        value = acc[4 * h + i]
        value = value * value
        sums[0, 1] += jnp.sum((value[:, :128] + value[:, 128:]).reshape(32, 8, 128), axis=0)
        return carry

    lax.fori_loop(0, 4, squares, 0)

    def sum_copy(phase, slot, device):
        return copy(sums.at[phase], sums_in.at[3 * phase + slot], S_SUM + 3 * phase + slot - (2 if phase else 0), device)

    def sum_copies(phase):
        if phase == 0:
            return [sum_copy(0, 0, partner)]
        make = (None, lambda j: dev(dx=j), dev_y, lambda j: dev(dz=j))[phase]
        return [sum_copy(phase, j - 1, make(j)) for j in range(1, 4)]

    for c in sum_copies(0):
        c.start()

    def mirror_row(j):
        dz, dy = j // 2, j % 2
        to_z, to_y = (z + dz) % 4, (yh + dy) % 2
        src = acc.at[4 * h + to_z, :, pl.ds(pl.multiple_of(to_y * 128, 128), 128)]
        return copy(src, m1.at[me_r], S_M1 + j, dev(dz=dz, dyh=dy))

    def mirror_row_in(j):
        from_z, from_y = (z + 4 - j // 2) % 4, (yh + j % 2) % 2
        ref = m1.at[from_z * 2 + from_y]
        return copy(ref, ref, S_M1 + j, zp)

    for j in range(1, 8):
        mirror_row(j).start()
    for side in range(2):
        @pl.when(yh == side)
        def _():
            m1[me_r] = acc[4 * h + z, :, side * 128:(side + 1) * 128]

    for phase in range(4):
        copies = sum_copies(phase)
        for c in copies:
            c.wait_recv()
        total = sums[phase]
        for slot in range(len(copies)):
            total += sums_in[3 * phase + slot]
        sums[phase + 1] = total
        if phase < 3:
            for c in sum_copies(phase + 1):
                c.start()

    def mirror_col(j):
        dx, dh = j // 2, j % 2
        to_x, to_h = (x + dx) % 4, (h + dh) % 2
        return copy(m1.at[to_x * 2 + to_h], m2.at[h, x], S_M2 + j, dev(dx=dx, dh=dh))

    def mirror_col_in(j):
        from_x, from_h = (x + 4 - j // 2) % 4, (h + j % 2) % 2
        ref = m2.at[from_h, from_x]
        return copy(ref, ref, S_M2 + j, xp)

    for j in range(1, 8):
        mirror_row_in(j).wait_recv()
    for j in range(1, 8):
        mirror_col(j).start()
    m2[h, x] = m1[x * 2 + h]

    load_top.wait()
    total = sums[4]
    ratio = jnp.sum(total[1], axis=(0, 1), keepdims=True) / jnp.sum(total[0], axis=(0, 1), keepdims=True)
    balance = jnp.sqrt(jnp.sqrt(ratio))
    half = 0.5 * balance
    inverse = -0.5 / balance
    for j in range(1, 8):
        mirror_col_in(j).wait_recv()
    for k in range(2):
        for m in range(8):
            block = m2[k, m // 2, (m % 2) * 128:(m % 2 + 1) * 128]
            where = pl.ds(m, 128, stride=8)
            out[k, where, :] = half * top[k, where, :] + inverse * block.T

    for step in range(1, 8):
        for side in range(2):
            below_copy(me_r, side, step, zp).wait_send()
    for side in range(2):
        copy(ball.at[me_r, side], yfwd.at[side], S_FWD + side, yp).wait_send()
    swap_l.wait_send()

    @pl.when(mine_l)
    def _():
        for c in spread_l(my_pair, S_L + 1, "x"):
            c.wait_send()
        for c in spread_l(lall.at[yl, yh, z], S_L + 4, "z"):
            c.wait_send()
        l_copy(7, 1).wait_send()
        l_copy(8, 3).wait_send()

    @pl.when(beside_l)
    def _():
        l_forward(9, 3, 1, 0).wait_send()
        l_forward(10, 1, 3, 2).wait_send()

    def last_y(s, carry):
        y_copy(s).wait_send()
        return carry

    lax.fori_loop(0, 8, last_y, 0)

    @pl.when(h == 1)
    def _():
        out_copy.wait_send()

    for j in range(1, 8):
        mirror_row(j).wait_send()
        mirror_col(j).wait_send()
    for phase in range(4):
        for c in sum_copies(phase):
            c.wait_send()


def per_device(matrix, inverse_rest, upper_block, lower_below, lower_inverse):
    vmem = pltpu.VMEM
    dma = pltpu.SemaphoreType.DMA
    result = pl.pallas_call(
        kernel,
        out_shape=jax.ShapeDtypeStruct((2, 1024, 128), F32),
        in_specs=[pl.BlockSpec(memory_space=ANY)] * 5,
        out_specs=pl.BlockSpec(memory_space=pltpu.VMEM),
        scratch_shapes=[
            vmem((8, 2, 7, 128, 128), F32),
            vmem((2, 7, 128, 128), F32),
            vmem((2048, 1792), BF16),
            vmem((256, 2688), BF16),
            vmem((4, 2, 2048, 128), F32),
            vmem((8, 2048, 128), F32),
            vmem((8, 2, 256, 128), F32),
            vmem((8, 2, 512, 128), F32),
            vmem((8, 256, 128), F32),
            vmem((8, 512, 128), F32),
            vmem((8, 256, 256), BF16),
            vmem((2, 2, 4, 4, 128, 256), F32),
            vmem((8, 256, 256), F32),
            vmem((4, 256, 256), F32),
            vmem((8, 256, 128), F32),
            vmem((2, 4, 256, 128), F32),
            vmem((2, 1024, 128), F32),
            vmem((2, 1024, 128), F32),
            vmem((2, 7, 128, 128), F32),
            vmem((2, 128, 128), F32),
            vmem((2, 128, 128), F32),
            vmem((5, 2, 8, 128), F32),
            vmem((12, 2, 8, 128), F32),
            dma((5,)),
            dma((2,)),
            dma((2,)),
            dma((N_SEM,)),
            dma((N_SEM,)),
        ],
        compiler_params=pltpu.CompilerParams(
            collective_id=0, has_side_effects=True, vmem_limit_bytes=67043328
        ),
    )(
        matrix.reshape(16, 1024, 128),
        inverse_rest.transpose(0, 2, 1, 3),
        upper_block.reshape(2, 128, 128),
        lower_below.transpose(0, 2, 1, 3),
        lower_inverse,
    )
    return result.reshape(2, 128, 8, 128)


def solution(mesh):
    split_mesh = Mesh(mesh.devices.reshape(4, 2, 2, 4, 2), ("row_0", "row_1", "col_0", "col_1", "col_2"))
    return jax.shard_map(
        per_device,
        mesh=split_mesh,
        in_specs=(
            P(None, ROW, None, COL),
            P(None, ROW, None, COL),
            P(None, ROW, None, COL),
            P(None, ROW, None, COL),
            P(None, ROW, COL),
        ),
        out_specs=P(None, ROW, None, COL),
        check_vma=False,
    )
```

```python
import jax
import jax.numpy as jnp
from jax import lax
from jax.experimental import pallas as pl
from jax.experimental.pallas import tpu as pltpu
from jax.sharding import Mesh
from jax.sharding import PartitionSpec as P

ROW = ("row_0", "row_1")
COL = ("col_0", "col_1", "col_2")
MESH = pl.DeviceIdType.MESH
F32 = jnp.float32
BF16 = jnp.bfloat16
ANY = pl.ANY

S_BELOW = 0
S_FWD = 16
S_PAIR = 18
S_A = 50
S_B = 66
S_Y = 82
S_L = 90
S_LY = 98
S_OUT = 146
S_M1 = 150
S_M2 = 158
S_SUM = 166
N_SEM = 176


def split(value):
    hi = value.astype(BF16)
    lo = (value - hi.astype(F32)).astype(BF16)
    return hi, lo


def dot_t(a, b):
    return lax.dot_general(a, b, (((1,), (1,)), ((), ())), preferred_element_type=F32)


def dot_n(a, b):
    return lax.dot_general(a, b, (((1,), (0,)), ((), ())), preferred_element_type=F32)


def rows_at(block, count):
    return pl.ds(pl.multiple_of(block * 128, 128), count * 128)


def kernel(
    mat, rest, up, below, linv, out,
    ball, yfwd, rcat, bcat, part, pair, rec_a, rec_b, rec_y, xy, xs, lall, lsplit, acc, acc_in,
    m1, m2, top, mstage, ublk, lstage, sums, sums_in,
    in_sem, r_sem, m_sem, send, recv,
):
    z = lax.axis_index("row_0")
    yh = lax.axis_index("row_1")
    yl = lax.axis_index("col_0")
    x = lax.axis_index("col_1")
    h = lax.axis_index("col_2")
    me_r = z * 2 + yh
    y = yh * 2 + yl

    def dev(dz=0, dyh=0, dyl=0, dx=0, dh=0):
        return ((z + dz) % 4, (yh + dyh) % 2, (yl + dyl) % 2, (x + dx) % 4, (h + dh) % 2)

    def dev_y(dy):
        there = (y + dy) % 4
        return (z, there // 2, there % 2, x, h)

    def copy(src, dst, index, device):
        return pltpu.make_async_remote_copy(
            src_ref=src, dst_ref=dst, send_sem=send.at[index], recv_sem=recv.at[index],
            device_id=device, device_id_type=MESH,
        )

    partner = dev(dh=1)
    zp, zm = dev(dz=1), dev(dz=3)
    xp, xm = dev(dx=1), dev(dx=3)
    yp, ym = dev_y(1), dev_y(3)
    ypair = dev(dyl=1)

    load_below = [pltpu.make_async_copy(below.at[k], ball.at[me_r, k], in_sem.at[k]) for k in range(2)]
    load_l = pltpu.make_async_copy(linv, lstage, in_sem.at[2])
    load_u = pltpu.make_async_copy(up, ublk, in_sem.at[3])
    load_top = pltpu.make_async_copy(mat.at[pl.ds(0, 2)], top, in_sem.at[4])

    def staged(p):
        return (p // 4, (p // 2) % 2, pl.ds(pl.multiple_of((p % 2) * 896, 128), 896))

    def load_r(p):
        return pltpu.make_async_copy(rest.at[p], part.at[staged(p)], r_sem.at[p])

    def load_m(p):
        return pltpu.make_async_copy(mat.at[p], mstage.at[p % 2], m_sem.at[p % 2])

    for load in (*load_below, load_l):
        load.start()
    for p in range(16):
        load_r(p).start()
    load_u.start()
    load_top.start()

    barrier = pltpu.get_barrier_semaphore()
    friends = [dev(dz=dz, dyh=dyh) for dz in range(4) for dyh in range(2) if (dz, dyh) != (0, 0)]
    friends += [dev(dx=dx, dh=dh) for dx in range(4) for dh in range(2) if (dx, dh) != (0, 0)]
    friends += [yp, ym]
    for friend in friends:
        pl.semaphore_signal(barrier, inc=1, device_id=friend, device_id_type=MESH)

    sums[...] = jnp.zeros(sums.shape, F32)

    def take_r(p, carry):
        load_r(p).wait()
        where = pl.ds(pl.multiple_of(((p // 4) * 4 + (p % 2) * 2 + (p // 2) % 2) * 128, 128), 128)
        total = jnp.zeros((8, 128), F32)
        for q in range(7):
            rows = pl.ds(pl.multiple_of((p % 2) * 896 + q * 128, 128), 128)
            value = part[p // 4, (p // 2) % 2, rows]
            total += jnp.sum((value * value).reshape(16, 8, 128), axis=0)
            hi, lo = split(value)
            rcat[where, q * 128:(q + 1) * 128] = hi
            rcat[where, (7 + q) * 128:(8 + q) * 128] = lo
        sums[0, 1] += total
        return carry

    lax.fori_loop(0, 8, take_r, 0)
    for load in load_below:
        load.wait()
    load_l.wait()
    pl.semaphore_wait(barrier, len(friends))

    def below_copy(source, half, step, device):
        ref = ball.at[source, half]
        return copy(ref, ref, S_BELOW + 2 * step + half, device)

    below_copy(me_r, 0, 1, zp).start()
    below_copy(me_r, 1, 2, zm).start()
    copy(ball.at[me_r, 0], yfwd.at[0], S_FWD, yp).start()
    copy(ball.at[me_r, 1], yfwd.at[1], S_FWD + 1, ym).start()

    my_l = lall.at[yl, yh, x, z]
    lanes = pl.ds(pl.multiple_of(h * 128, 128), 128)
    swap_l = copy(lstage.at[1 - h], lall.at[yl, yh, x, z, :, lanes], S_L, partner)
    swap_l.start()
    for core in range(2):
        @pl.when(h == core)
        def _():
            lall[yl, yh, x, z, :, core * 128:(core + 1) * 128] = lstage[core]

    lax.fori_loop(8, 16, take_r, 0)
    load_u.wait()

    mine_l = jnp.logical_or(h == 1, yl == 0)
    beside_l = jnp.logical_or(h == 1, yl == 1)
    swap_l.wait_recv()

    def lz_copies():
        return [copy(my_l, my_l, S_L + j, dev(dz=j)) for j in range(1, 4)]

    def lx_copy(side):
        ref = lall.at[yl, yh, x]
        return copy(ref, ref, S_L + 4 + side, xp if side == 0 else xm)

    def lx_forward(side):
        ref = lall.at[yl, yh, (x + (3 if side == 0 else 1)) % 4, pl.ds(2 * side, 2)]
        return copy(ref, ref, S_L + 6 + side, xp if side == 0 else xm)

    @pl.when(mine_l)
    def _():
        for c in lz_copies():
            c.start()

    below_copy(me_r, 1, 1, zp).start()
    below_copy(me_r, 0, 2, zm).start()

    def ly_copy(side, from_dy, xq, zq):
        there = (y + from_dy) % 4
        ref = lall.at[there % 2, there // 2, xq, zq]
        if side == 2:
            even = (xq + zq) % 2 == 0
            target = (y + jnp.where(even, 1, 3)) % 4
            device = (z, target // 2, target % 2, x, h)
        else:
            device = yp if side == 0 else ym
        return copy(ref, ref, S_LY + 16 * side + xq * 4 + zq, device)

    def needed(yl_from, xq, zq):
        return jnp.logical_or(h != yl_from, xq <= zq)

    def ly_each(dx, yl_from, fn):
        xq = (x + dx) % 4
        for zq in range(4):
            @pl.when(needed(yl_from, xq, zq))
            def _():
                fn(xq, zq)

    def ly_start(dx):
        @pl.when(mine_l)
        def _():
            def fn(xq, zq):
                ly_copy(0, 0, xq, zq).start()
                ly_copy(1, 0, xq, zq).start()

            ly_each(dx, yl, fn)

    def ly_forward(dx):
        @pl.when(beside_l)
        def _():
            def fn(xq, zq):
                ly_copy(0, 3, xq, zq).wait_recv()
                ly_copy(1, 1, xq, zq).wait_recv()
                from_dy = jnp.where((xq + zq) % 2 == 0, 3, 1)
                ly_copy(2, from_dy, xq, zq).start()

            ly_each(dx, 1 - yl, fn)

    def source(step):
        dz = jnp.where(jnp.logical_or(step == 1, step == 5), 3, jnp.where(jnp.logical_or(step == 2, step == 6), 1, 0))
        dz = jnp.where(jnp.logical_or(step == 4, step == 7), 2, dz)
        dy = jnp.where(jnp.logical_or(step == 3, step >= 5), 1, 0)
        return (z + dz) % 4, (yh + dy) % 2

    def source_row(step):
        zs, ys = source(step)
        return zs * 2 + ys

    def pair_copy(s, share):
        where = rows_at(share * 4, 4)
        return copy(part.at[s % 4, 1 - h, where], pair.at[s, where], S_PAIR + 4 * s + share, partner)

    def add_pair(s, share):
        pair_copy(s, share).wait_recv()

        def add(i, carry):
            where = rows_at(share * 4 + i, 1)
            part[s % 4, h, where] += pair[s, where]
            return carry

        lax.fori_loop(0, 4, add, 0)

    def a_copy(s, side):
        far = (x + 2) % 4
        src = part.at[s % 4, h, rows_at(far * 4 + 2 * side, 2)]
        return copy(src, rec_a.at[s, side], S_A + 2 * s + side, xp if side == 0 else xm)

    def b_copy(s, side):
        near = (x + (1 if side == 0 else 3)) % 4
        src = part.at[s % 4, h, rows_at(near * 4, 4)]
        return copy(src, rec_b.at[s, side], S_B + 2 * s + side, xp if side == 0 else xm)

    def y_copy(s):
        return copy(xy.at[s, rows_at((1 - yl) * 2, 2)], rec_y.at[s], S_Y + s, ypair)

    def step_body(t, carry):
        @pl.when(t < 8)
        def _():
            load_m(2 * t).start()
            load_m(2 * t + 1).start()

        @pl.when(t == 1)
        def _():
            below_copy(source_row(1), 0, 1, zp).wait_recv()
            below_copy(source_row(1), 0, 4, zp).start()
            below_copy(source_row(2), 1, 2, zm).wait_recv()
            below_copy(source_row(2), 1, 4, zm).start()

        @pl.when(t == 2)
        def _():
            @pl.when(mine_l)
            def _():
                for c in lz_copies():
                    c.wait_recv()
                lx_copy(0).start()
                lx_copy(1).start()

            ly_start(0)

        @pl.when(t == 3)
        def _():
            r = source_row(3)
            below_copy(r, 0, 3, zp).wait_recv()
            below_copy(r, 1, 3, zp).wait_recv()
            below_copy(r, 0, 5, zp).start()
            below_copy(r, 1, 6, zm).start()
            below_copy(r, 1, 5, zp).start()
            below_copy(r, 0, 6, zm).start()

        @pl.when(t == 4)
        def _():
            @pl.when(mine_l)
            def _():
                lx_copy(0).wait_recv()
                lx_forward(0).start()
                lx_copy(1).wait_recv()
                lx_forward(1).start()

            ly_start(1)
            ly_start(3)
            ly_forward(0)

        @pl.when(t == 5)
        def _():
            below_copy(source_row(5), 0, 5, zp).wait_recv()
            below_copy(source_row(5), 0, 7, zp).start()
            below_copy(source_row(6), 1, 6, zm).wait_recv()
            below_copy(source_row(6), 1, 7, zm).start()

            @pl.when(mine_l)
            def _():
                lx_forward(0).wait_recv()
                lx_forward(1).wait_recv()

            ly_start(2)

        @pl.when(t == 7)
        def _():
            ly_forward(1)
            ly_forward(3)

        @pl.when(t < 8)
        def _():
            r = source_row(t)
            seen = jnp.logical_or(t == 0, t == 3)
            seen0 = jnp.logical_or(seen, jnp.logical_or(t == 1, t == 5))
            seen1 = jnp.logical_or(seen, jnp.logical_or(t == 2, t == 6))

            @pl.when(jnp.logical_not(seen0))
            def _():
                below_copy(r, 0, t, zp).wait_recv()

            @pl.when(jnp.logical_not(seen1))
            def _():
                below_copy(r, 1, t, zp).wait_recv()

            for k in range(2):
                for q in range(7):
                    hi, lo = split(ball[r, k, q])
                    where = slice(k * 128, (k + 1) * 128)
                    bcat[where, q * 128:(q + 1) * 128] = hi
                    bcat[where, (7 + q) * 128:(8 + q) * 128] = hi
                    bcat[where, (14 + q) * 128:(15 + q) * 128] = lo

            def quarter(i, carry):
                share = (x + 2 + i) % 4
                for u in range(2):
                    where = rows_at(share * 4 + 2 * u, 2)
                    value = dot_t(rcat[where, 0:1792], bcat[:, 0:1792]) + dot_t(rcat[where, 0:896], bcat[:, 1792:2688])
                    part[t % 4, 0, where] = value[:, :128]
                    part[t % 4, 1, where] = value[:, 128:]

                @pl.when(jnp.logical_and((yl * 8 + x * 2 + h) % 8 == r, share == 0))
                def _():
                    for k in range(2):
                        part[t % 4, yl, k * 256:k * 256 + 128] -= ublk[k]

                pair_copy(t, share).start()
                return carry

            lax.fori_loop(0, 4, quarter, 0)

            for slot in range(2):
                load_m(2 * t + slot).wait()
                value = mstage[slot]
                sums[0, 0] += jnp.sum((value * value).reshape(128, 8, 128), axis=0)

            add_pair(t, (x + 2) % 4)
            a_copy(t, 0).start()
            a_copy(t, 1).start()

        @pl.when(t == 0)
        def _():
            copy(yfwd.at[0], yfwd.at[0], S_FWD, yp).wait_recv()
            copy(yfwd.at[1], yfwd.at[1], S_FWD + 1, ym).wait_recv()
            back = (y + 3) % 4
            copy(yfwd.at[0], ball.at[z * 2 + back // 2, 0], S_BELOW + 6, yp).start()
            ahead = (y + 1) % 4
            copy(yfwd.at[1], ball.at[z * 2 + ahead // 2, 1], S_BELOW + 7, ym).start()

        @pl.when(jnp.logical_and(t >= 1, t < 9))
        def _():
            s = t - 1
            for side in range(2):
                near = (x + (1 if side == 0 else 3)) % 4
                add_pair(s, near)
                a_copy(s, side).wait_recv()
                where = rows_at(near * 4 + 2 * side, 2)
                part[s % 4, h, where] += rec_a[s, side]
                b_copy(s, side).start()
            add_pair(s, x)

        @pl.when(t >= 2)
        def _():
            s = t - 2
            b_copy(s, 0).wait_recv()
            b_copy(s, 1).wait_recv()

            def add(i, carry):
                where = rows_at(i, 1)
                xy[s, where] = part[s % 4, h, rows_at(x * 4 + i, 1)] + rec_b[s, 0, where] + rec_b[s, 1, where]
                return carry

            lax.fori_loop(0, 4, add, 0)
            y_copy(s).start()
            for share in range(4):
                pair_copy(s, share).wait_send()
            for side in range(2):
                a_copy(s, side).wait_send()
                b_copy(s, side).wait_send()

        return carry

    lax.fori_loop(0, 10, step_body, 0)

    ly_forward(2)

    def take_y(s, carry):
        y_copy(s).wait_recv()
        hi, lo = split(xy[s, rows_at(yl * 2, 2)] + rec_y[s])
        xs[0, source_row(s)] = hi
        xs[1, source_row(s)] = lo
        return carry

    lax.fori_loop(0, 8, take_y, 0)

    def ly_last(fn):
        @pl.when(mine_l)
        def _():
            for dx in range(4):
                ly_each(dx, yl, fn)

    ly_last(lambda xq, zq: ly_copy(2, 2, xq, zq).wait_recv())

    def product(i):
        for r in range(8):
            piece = lall[i // 4, r % 2, i % 4, r // 2]
            hi, lo = split(jnp.where(needed(i // 4, i % 4, r // 2), piece, 0.0))
            lsplit[0, r * 128:(r + 1) * 128] = hi
            lsplit[1, r * 128:(r + 1) * 128] = lo
        left = jnp.concatenate([xs[0, r] for r in range(8)], axis=1)
        rest_of = jnp.concatenate([xs[1, r] for r in range(8)], axis=1)
        acc[i] = dot_n(left, lsplit[0]) + dot_n(rest_of, lsplit[0]) + dot_n(left, lsplit[1])

    def out_copy(i):
        return copy(acc.at[i], acc_in.at[i], S_OUT + i, partner)

    def mirror_row(j, side):
        to_z = (z + j) % 4
        src = acc.at[4 * h + to_z, :, side * 128:(side + 1) * 128]
        other = jnp.where(yh == side, 0, 1)
        return copy(src, m1.at[me_r], S_M1 + 2 * j + other, (to_z, side, yl, x, h))

    def mirror_row_in(j, other):
        from_z, from_y = (z + 4 - j) % 4, (yh + other) % 2
        ref = m1.at[from_z * 2 + from_y]
        return copy(ref, ref, S_M1 + 2 * j + other, zp)

    @pl.when(h == 1)
    def _():
        def early(j, carry):
            i = (z + 1 + j) % 4
            product(i)
            out_copy(i).start()
            return carry

        lax.fori_loop(0, 4, early, 0)

    def late(j0, carry):
        j = (j0 + 1) % 4
        i = (z + j) % 4
        product(4 * h + i)

        @pl.when(h == 0)
        def _():
            out_copy(i).wait_recv()
            acc[i] += acc_in[i]

        value = acc[4 * h + i]
        value = value * value
        sums[0, 1] += jnp.sum((value[:, :128] + value[:, 128:]).reshape(32, 8, 128), axis=0)
        for side in range(2):
            @pl.when(jnp.logical_or(j != 0, yh != side))
            def _():
                mirror_row(j, side).start()

            @pl.when(jnp.logical_and(j == 0, yh == side))
            def _():
                m1[me_r] = acc[4 * h + z, :, side * 128:(side + 1) * 128]

        return carry

    lax.fori_loop(0, 4, late, 0)

    def sum_copy(phase, slot, device):
        return copy(sums.at[phase], sums_in.at[3 * phase + slot], S_SUM + 3 * phase + slot - (2 if phase else 0), device)

    def sum_copies(phase):
        if phase == 0:
            return [sum_copy(0, 0, partner)]
        make = (None, lambda j: dev(dx=j), dev_y, lambda j: dev(dz=j))[phase]
        return [sum_copy(phase, j - 1, make(j)) for j in range(1, 4)]

    for c in sum_copies(0):
        c.start()

    for phase in range(4):
        copies = sum_copies(phase)
        for c in copies:
            c.wait_recv()
        total = sums[phase]
        for slot in range(len(copies)):
            total += sums_in[3 * phase + slot]
        sums[phase + 1] = total
        if phase < 3:
            for c in sum_copies(phase + 1):
                c.start()

    def mirror_col(to_x, to_h):
        index = S_M2 + 2 * ((to_x + 4 - x) % 4) + (to_h + h) % 2
        return copy(m1.at[to_x * 2 + to_h], m2.at[h, x], index, (z, yh, yl, to_x, to_h))

    def mirror_col_in(j):
        from_x, from_h = (x + 4 - j // 2) % 4, (h + j % 2) % 2
        ref = m2.at[from_h, from_x]
        return copy(ref, ref, S_M2 + j, xp)

    def spread(j, carry):
        from_z, from_y = (z + 4 - j // 2) % 4, (yh + j % 2) % 2

        @pl.when(j > 0)
        def _():
            mirror_row_in(j // 2, j % 2).wait_recv()

        here = jnp.logical_and(from_z == x, from_y == h)

        @pl.when(here)
        def _():
            m2[h, x] = m1[x * 2 + h]

        @pl.when(jnp.logical_not(here))
        def _():
            mirror_col(from_z, from_y).start()

        return carry

    lax.fori_loop(0, 8, spread, 0)

    load_top.wait()
    total = sums[4]
    ratio = jnp.sum(total[1], axis=(0, 1), keepdims=True) / jnp.sum(total[0], axis=(0, 1), keepdims=True)
    balance = jnp.sqrt(jnp.sqrt(ratio))
    half = 0.5 * balance
    inverse = -0.5 / balance

    def finish(j, carry):
        @pl.when(j > 0)
        def _():
            mirror_col_in(j).wait_recv()

        k, xf = (h + j % 2) % 2, (x + 4 - j // 2) % 4
        for m in range(2):
            block = m2[k, xf, m * 128:(m + 1) * 128]
            where = pl.ds(2 * xf + m, 128, stride=8)
            out[k, where, :] = half * top[k, where, :] + inverse * block.T
        return carry

    lax.fori_loop(0, 8, finish, 0)

    for step in range(1, 8):
        for side in range(2):
            below_copy(me_r, side, step, zp).wait_send()
    for side in range(2):
        copy(ball.at[me_r, side], yfwd.at[side], S_FWD + side, yp).wait_send()
    swap_l.wait_send()

    @pl.when(mine_l)
    def _():
        for c in lz_copies():
            c.wait_send()
        for side in range(2):
            lx_copy(side).wait_send()
            lx_forward(side).wait_send()

    def ly_sent(xq, zq):
        ly_copy(0, 0, xq, zq).wait_send()
        ly_copy(1, 0, xq, zq).wait_send()

    ly_last(ly_sent)

    @pl.when(beside_l)
    def _():
        for dx in range(4):
            ly_each(dx, 1 - yl, lambda xq, zq: ly_copy(2, 1, xq, zq).wait_send())

    def last_y(s, carry):
        y_copy(s).wait_send()
        return carry

    lax.fori_loop(0, 8, last_y, 0)

    @pl.when(h == 1)
    def _():
        for i in range(4):
            out_copy(i).wait_send()

    def last_mirror(j, carry):
        copy(m1.at[0], m1.at[0], S_M1 + j, zp).wait_send()
        copy(m1.at[0], m1.at[0], S_M2 + j, xp).wait_send()
        return carry

    lax.fori_loop(1, 8, last_mirror, 0)
    for phase in range(4):
        for c in sum_copies(phase):
            c.wait_send()


def per_device(matrix, inverse_rest, upper_block, lower_below, lower_inverse):
    vmem = pltpu.VMEM
    dma = pltpu.SemaphoreType.DMA
    result = pl.pallas_call(
        kernel,
        out_shape=jax.ShapeDtypeStruct((2, 1024, 128), F32),
        in_specs=[pl.BlockSpec(memory_space=ANY)] * 5,
        out_specs=pl.BlockSpec(memory_space=pltpu.VMEM),
        scratch_shapes=[
            vmem((8, 2, 7, 128, 128), F32),
            vmem((2, 7, 128, 128), F32),
            vmem((2048, 1792), BF16),
            vmem((256, 2688), BF16),
            vmem((4, 2, 2048, 128), F32),
            vmem((8, 2048, 128), F32),
            vmem((8, 2, 256, 128), F32),
            vmem((8, 2, 512, 128), F32),
            vmem((8, 256, 128), F32),
            vmem((8, 512, 128), F32),
            vmem((2, 8, 256, 128), BF16),
            vmem((2, 2, 4, 4, 128, 256), F32),
            vmem((2, 1024, 256), BF16),
            vmem((8, 256, 256), F32),
            vmem((4, 256, 256), F32),
            vmem((8, 256, 128), F32),
            vmem((2, 4, 256, 128), F32),
            vmem((2, 1024, 128), F32),
            vmem((2, 1024, 128), F32),
            vmem((2, 128, 128), F32),
            vmem((2, 128, 128), F32),
            vmem((5, 2, 8, 128), F32),
            vmem((12, 2, 8, 128), F32),
            dma((5,)),
            dma((16,)),
            dma((2,)),
            dma((N_SEM,)),
            dma((N_SEM,)),
        ],
        compiler_params=pltpu.CompilerParams(
            collective_id=0, has_side_effects=True, vmem_limit_bytes=67043328
        ),
    )(
        matrix.reshape(16, 1024, 128),
        inverse_rest.transpose(0, 2, 1, 3).reshape(16, 896, 128),
        upper_block.reshape(2, 128, 128),
        lower_below.transpose(0, 2, 1, 3),
        lower_inverse,
    )
    return result.reshape(2, 128, 8, 128)


def solution(mesh):
    split_mesh = Mesh(mesh.devices.reshape(4, 2, 2, 4, 2), ("row_0", "row_1", "col_0", "col_1", "col_2"))
    return jax.shard_map(
        per_device,
        mesh=split_mesh,
        in_specs=(
            P(None, ROW, None, COL),
            P(None, ROW, None, COL),
            P(None, ROW, None, COL),
            P(None, ROW, None, COL),
            P(None, ROW, COL),
        ),
        out_specs=P(None, ROW, None, COL),
        check_vma=False,
    )
```

```python
import jax
import jax.numpy as jnp
from jax import lax
from jax.experimental import pallas as pl
from jax.experimental.pallas import tpu as pltpu
from jax.sharding import Mesh
from jax.sharding import PartitionSpec as P

ROW = ("row_0", "row_1")
COL = ("col_0", "col_1", "col_2")
MESH = pl.DeviceIdType.MESH
F32 = jnp.float32
BF16 = jnp.bfloat16
ANY = pl.ANY

S_BELOW = 0
S_FWD = 16
S_PAIR = 18
S_A = 50
S_B = 66
S_Y = 82
S_L = 90
S_L2 = 94
S_LY = 106
S_OUT = 154
S_M1 = 158
S_M2 = 166
S_MF = 174
S_SUM = 177
N_SEM = 199


def split(value):
    hi = value.astype(BF16)
    lo = (value - hi.astype(F32)).astype(BF16)
    return hi, lo


def dot_t(a, b):
    return lax.dot_general(a, b, (((1,), (1,)), ((), ())), preferred_element_type=F32)


def dot_n(a, b):
    return lax.dot_general(a, b, (((1,), (0,)), ((), ())), preferred_element_type=F32)


def rows_at(block, count):
    return pl.ds(pl.multiple_of(block * 128, 128), count * 128)


def kernel(
    mat, rest, up, below, linv, out,
    ball, yfwd, rcat, bcat, part, pair, rec_a, rec_b, rec_y, xy, xs, lall, lsplit, acc, acc_in,
    m1, m2, mfwd, top, mstage, ublk, lstage, sums, sums_in,
    in_sem, r_sem, m_sem, send, recv,
):
    z = lax.axis_index("row_0")
    yh = lax.axis_index("row_1")
    yl = lax.axis_index("col_0")
    x = lax.axis_index("col_1")
    h = lax.axis_index("col_2")
    me_r = z * 2 + yh
    y = yh * 2 + yl

    def dev(dz=0, dyh=0, dyl=0, dx=0, dh=0):
        return ((z + dz) % 4, (yh + dyh) % 2, (yl + dyl) % 2, (x + dx) % 4, (h + dh) % 2)

    def dev_y(dy):
        there = (y + dy) % 4
        return (z, there // 2, there % 2, x, h)

    def copy(src, dst, index, device):
        return pltpu.make_async_remote_copy(
            src_ref=src, dst_ref=dst, send_sem=send.at[index], recv_sem=recv.at[index],
            device_id=device, device_id_type=MESH,
        )

    partner = dev(dh=1)
    zp, zm = dev(dz=1), dev(dz=3)
    xp, xm = dev(dx=1), dev(dx=3)
    yp, ym = dev_y(1), dev_y(3)
    ypair = dev(dyl=1)

    load_below = [pltpu.make_async_copy(below.at[k], ball.at[me_r, k], in_sem.at[k]) for k in range(2)]
    load_l = pltpu.make_async_copy(linv, lstage, in_sem.at[2])
    load_u = pltpu.make_async_copy(up, ublk, in_sem.at[3])
    load_top = pltpu.make_async_copy(mat.at[pl.ds(0, 2)], top, in_sem.at[4])

    def staged(p):
        return (p // 4, (p // 2) % 2, pl.ds(pl.multiple_of((p % 2) * 896, 128), 896))

    def load_r(p):
        return pltpu.make_async_copy(rest.at[p], part.at[staged(p)], r_sem.at[p])

    def load_m(p):
        return pltpu.make_async_copy(mat.at[p], mstage.at[p % 2], m_sem.at[p % 2])

    for load in (*load_below, load_l):
        load.start()
    for p in range(16):
        load_r(p).start()
    load_u.start()
    load_top.start()

    barrier = pltpu.get_barrier_semaphore()
    def dev_zy(dz, dy):
        there = (y + dy) % 4
        return ((z + dz) % 4, there // 2, there % 2, x, h)

    friends = [dev_zy(j // 4, j % 4) for j in range(1, 16)]
    friends += [dev(dx=j // 2, dh=j % 2) for j in range(1, 8)]
    for friend in friends:
        pl.semaphore_signal(barrier, inc=1, device_id=friend, device_id_type=MESH)

    sums[...] = jnp.zeros(sums.shape, F32)

    def take_r(p, carry):
        load_r(p).wait()
        where = pl.ds(pl.multiple_of(((p // 4) * 4 + (p % 2) * 2 + (p // 2) % 2) * 128, 128), 128)
        total = jnp.zeros((8, 128), F32)
        for q in range(7):
            rows = pl.ds(pl.multiple_of((p % 2) * 896 + q * 128, 128), 128)
            value = part[p // 4, (p // 2) % 2, rows]
            total += jnp.sum((value * value).reshape(16, 8, 128), axis=0)
            hi, lo = split(value)
            rcat[where, q * 128:(q + 1) * 128] = hi
            rcat[where, (7 + q) * 128:(8 + q) * 128] = lo
        sums[0, 1] += total
        return carry

    lax.fori_loop(0, 8, take_r, 0)
    for load in load_below:
        load.wait()
    load_l.wait()
    pl.semaphore_wait(barrier, len(friends))

    def below_copy(source, half, step, device):
        ref = ball.at[source, half]
        return copy(ref, ref, S_BELOW + 2 * step + half, device)

    below_copy(me_r, 0, 1, zp).start()
    below_copy(me_r, 1, 1, zm).start()
    copy(ball.at[me_r, 0], yfwd.at[0], S_FWD, yp).start()
    copy(ball.at[me_r, 1], yfwd.at[1], S_FWD + 1, ym).start()

    my_l = lall.at[yl, yh, x, z]
    lanes = pl.ds(pl.multiple_of(h * 128, 128), 128)
    swap_l = copy(lstage.at[1 - h], lall.at[yl, yh, x, z, :, lanes], S_L, partner)
    swap_l.start()
    for core in range(2):
        @pl.when(h == core)
        def _():
            lall[yl, yh, x, z, :, core * 128:(core + 1) * 128] = lstage[core]

    lax.fori_loop(8, 16, take_r, 0)
    load_u.wait()

    mine_l = jnp.logical_or(h == 1, yl == 0)
    beside_l = jnp.logical_or(h == 1, yl == 1)
    swap_l.wait_recv()

    def piece_at(i, d):
        return jnp.where(h == 0, (x + d) % 4, i), jnp.where(h == 0, i, (z + d) % 4)

    def dev_first(d):
        return (jnp.where(h == 0, (z + d) % 4, z), yh, yl, jnp.where(h == 0, x, (x + d) % 4), h)

    def dev_second(d):
        return (jnp.where(h == 0, z, (z + d) % 4), yh, yl, jnp.where(h == 0, (x + d) % 4, x), h)

    def needed(yl_from, xq, zq):
        return jnp.logical_or(h != yl_from, xq <= zq)

    def l1_copy(j):
        return copy(my_l, my_l, S_L + j, dev_first(j))

    def l1_wait(j):
        @pl.when(needed(yl, jnp.where(h == 0, x, (x + 4 - j) % 4), jnp.where(h == 0, (z + 4 - j) % 4, z)))
        def _():
            l1_copy(j).wait_recv()

    def l2_copy(side, i):
        xq, zq = piece_at(i, 0)
        ref = lall.at[yl, yh, xq, zq]
        return copy(ref, ref, S_L2 + 4 * side + i, dev_second(1 if side == 0 else 3))

    def l2_forward(i):
        xq, zq = piece_at(i, 3 if i % 2 == 0 else 1)
        ref = lall.at[yl, yh, xq, zq]
        return copy(ref, ref, S_L2 + 8 + i, dev_second(1 if i % 2 == 0 else 3))

    def l_each(d, yl_from, fn):
        for i in range(4):
            xq, zq = piece_at(i, d)

            def one(i=i, xq=xq, zq=zq):
                fn(i, xq, zq)

            pl.when(needed(yl_from, xq, zq))(one)

    def ly_copy(side, xq, zq):
        if side == 2:
            there = (y + jnp.where(yl == 1, 3, 1)) % 4
            target = (y + jnp.where(yl == 1, 1, 3)) % 4
            ref = lall.at[there % 2, there // 2, xq, zq]
            device = (z, target // 2, target % 2, x, h)
        else:
            ref = lall.at[yl, yh, xq, zq]
            device = yp if side == 0 else ym
        return copy(ref, ref, S_LY + 16 * side + xq * 4 + zq, device)

    def ly_start(d):
        @pl.when(mine_l)
        def _():
            def fn(i, xq, zq):
                ly_copy(0, xq, zq).start()
                ly_copy(1, xq, zq).start()

            l_each(d, yl, fn)

    def ly_forward(d):
        @pl.when(beside_l)
        def _():
            def fn(i, xq, zq):
                ly_copy(0, xq, zq).wait_recv()
                ly_copy(1, xq, zq).wait_recv()
                ly_copy(2, xq, zq).start()

            l_each(d, 1 - yl, fn)

    @pl.when(jnp.logical_and(mine_l, needed(yl, x, z)))
    def _():
        for j in range(1, 4):
            l1_copy(j).start()

    below_copy(me_r, 1, 2, zp).start()
    below_copy(me_r, 0, 2, zm).start()

    def source(step, half):
        late = jnp.logical_or(step == 3, step >= 5)
        down = jnp.logical_or(step == 1, step == 5)
        up = jnp.logical_or(step == 2, step == 6)
        dz = jnp.where(down, 3 - 2 * half, jnp.where(up, 1 + 2 * half, 0))
        dz = jnp.where(jnp.logical_or(step == 4, step == 7), 2, dz)
        return ((z + dz) % 4) * 2 + (yh + jnp.where(late, 1, 0)) % 2

    def pair_copy(s, share):
        where = rows_at(share * 4, 4)
        return copy(part.at[s % 4, 1 - h, where], pair.at[s, where], S_PAIR + 4 * s + share, partner)

    def add_pair(s, share):
        pair_copy(s, share).wait_recv()

        def add(i, carry):
            where = rows_at(share * 4 + i, 1)
            part[s % 4, h, where] += pair[s, where]
            return carry

        lax.fori_loop(0, 4, add, 0)

    def a_copy(s, side):
        far = (x + 2) % 4
        src = part.at[s % 4, h, rows_at(far * 4 + 2 * side, 2)]
        return copy(src, rec_a.at[s, side], S_A + 2 * s + side, xp if side == 0 else xm)

    def b_copy(s, side):
        near = (x + (1 if side == 0 else 3)) % 4
        src = part.at[s % 4, h, rows_at(near * 4, 4)]
        return copy(src, rec_b.at[s, side], S_B + 2 * s + side, xp if side == 0 else xm)

    def y_copy(s):
        return copy(xy.at[s, rows_at((1 - yl) * 2, 2)], rec_y.at[s], S_Y + s, ypair)

    def step_body(t, carry):
        @pl.when(t < 8)
        def _():
            load_m(2 * t).start()
            load_m(2 * t + 1).start()

        @pl.when(jnp.logical_and(t > 0, t < 8))
        def _():
            for k in range(2):
                below_copy(source(t, k), k, t, zp).wait_recv()

        @pl.when(t == 1)
        def _():
            below_copy(source(1, 0), 0, 4, zp).start()
            below_copy(source(1, 1), 1, 4, zm).start()

        @pl.when(t == 2)
        def _():
            @pl.when(mine_l)
            def _():
                for j in range(1, 4):
                    l1_wait(j)

                def fn(i, xq, zq):
                    l2_copy(0, i).start()
                    l2_copy(1, i).start()

                l_each(0, yl, fn)

            ly_start(0)

        @pl.when(t == 3)
        def _():
            r = source(3, 0)
            below_copy(r, 0, 5, zp).start()
            below_copy(r, 1, 5, zm).start()
            below_copy(r, 1, 6, zp).start()
            below_copy(r, 0, 6, zm).start()

        @pl.when(t == 4)
        def _():
            @pl.when(mine_l)
            def _():
                def from_down(i, xq, zq):
                    l2_copy(0, i).wait_recv()
                    if i % 2 == 0:
                        l2_forward(i).start()

                def from_up(i, xq, zq):
                    l2_copy(1, i).wait_recv()
                    if i % 2 == 1:
                        l2_forward(i).start()

                l_each(3, yl, from_down)
                l_each(1, yl, from_up)

            ly_start(1)
            ly_start(3)

        @pl.when(t == 5)
        def _():
            below_copy(source(5, 0), 0, 7, zp).start()
            below_copy(source(5, 1), 1, 7, zm).start()

            ly_forward(0)

        @pl.when(t == 6)
        def _():
            @pl.when(mine_l)
            def _():
                l_each(2, yl, lambda i, xq, zq: l2_forward(i).wait_recv())

            ly_start(2)

        @pl.when(t == 8)
        def _():
            ly_forward(1)
            ly_forward(3)

        @pl.when(t < 8)
        def _():
            for k in range(2):
                for q in range(7):
                    hi, lo = split(ball[source(t, k), k, q])
                    where = slice(k * 128, (k + 1) * 128)
                    bcat[where, q * 128:(q + 1) * 128] = hi
                    bcat[where, (7 + q) * 128:(8 + q) * 128] = hi
                    bcat[where, (14 + q) * 128:(15 + q) * 128] = lo

            def quarter(i, carry):
                share = (x + 2 + i) % 4
                for u in range(2):
                    where = rows_at(share * 4 + 2 * u, 2)
                    value = dot_t(rcat[where, 0:1792], bcat[:, 0:1792]) + dot_t(rcat[where, 0:896], bcat[:, 1792:2688])
                    part[t % 4, 0, where] = value[:, :128]
                    part[t % 4, 1, where] = value[:, 128:]

                @pl.when(jnp.logical_and(x * 2 + h == source(t, yl), share == 0))
                def _():
                    for k in range(2):
                        part[t % 4, yl, k * 256:k * 256 + 128] -= ublk[k]

                pair_copy(t, share).start()
                return carry

            lax.fori_loop(0, 4, quarter, 0)

            for slot in range(2):
                load_m(2 * t + slot).wait()
                value = mstage[slot]
                sums[0, 0] += jnp.sum((value * value).reshape(128, 8, 128), axis=0)

            add_pair(t, (x + 2) % 4)
            a_copy(t, 0).start()
            a_copy(t, 1).start()

        @pl.when(t == 0)
        def _():
            copy(yfwd.at[0], yfwd.at[0], S_FWD, yp).wait_recv()
            copy(yfwd.at[1], yfwd.at[1], S_FWD + 1, ym).wait_recv()
            back = (y + 3) % 4
            copy(yfwd.at[0], ball.at[z * 2 + back // 2, 0], S_BELOW + 6, yp).start()
            ahead = (y + 1) % 4
            copy(yfwd.at[1], ball.at[z * 2 + ahead // 2, 1], S_BELOW + 7, ym).start()

        @pl.when(jnp.logical_and(t >= 1, t < 9))
        def _():
            s = t - 1
            for side in range(2):
                near = (x + (1 if side == 0 else 3)) % 4
                add_pair(s, near)
                a_copy(s, side).wait_recv()
                where = rows_at(near * 4 + 2 * side, 2)
                part[s % 4, h, where] += rec_a[s, side]
                b_copy(s, side).start()
            add_pair(s, x)

        @pl.when(t >= 2)
        def _():
            s = t - 2
            b_copy(s, 0).wait_recv()
            b_copy(s, 1).wait_recv()

            def add(i, carry):
                where = rows_at(i, 1)
                xy[s, where] = part[s % 4, h, rows_at(x * 4 + i, 1)] + rec_b[s, 0, where] + rec_b[s, 1, where]
                return carry

            lax.fori_loop(0, 4, add, 0)
            y_copy(s).start()
            for share in range(4):
                pair_copy(s, share).wait_send()
            for side in range(2):
                a_copy(s, side).wait_send()
                b_copy(s, side).wait_send()

        return carry

    lax.fori_loop(0, 10, step_body, 0)

    ly_forward(2)

    def take_y(s, carry):
        y_copy(s).wait_recv()
        hi, lo = split(xy[s, rows_at(yl * 2, 2)] + rec_y[s])
        xs[0, source(s, h)] = hi
        xs[1, source(s, h)] = lo
        return carry

    lax.fori_loop(0, 8, take_y, 0)

    def ly_last(yl_from, fn):
        for d in range(4):
            l_each(d, yl_from, fn)

    @pl.when(mine_l)
    def _():
        ly_last(yl, lambda i, xq, zq: ly_copy(2, xq, zq).wait_recv())

    def product(i):
        for r in range(8):
            piece = lall[i // 4, r % 2, i % 4, r // 2]
            hi, lo = split(jnp.where(needed(i // 4, i % 4, r // 2), piece, 0.0))
            lsplit[0, r * 128:(r + 1) * 128] = hi
            lsplit[1, r * 128:(r + 1) * 128] = lo
        left = jnp.concatenate([xs[0, r] for r in range(8)], axis=1)
        rest_of = jnp.concatenate([xs[1, r] for r in range(8)], axis=1)
        acc[i] = dot_n(left, lsplit[0]) + dot_n(rest_of, lsplit[0]) + dot_n(left, lsplit[1])

    def out_copy(i):
        return copy(acc.at[i], acc_in.at[i], S_OUT + i, partner)

    def mirror_row(j, side, other):
        to_z = (z + j) % 4
        src = acc.at[4 * h + to_z, :, side * 128:(side + 1) * 128]
        if other and j == 0:
            return copy(src, mfwd.at[0], S_MF, ym)
        if other and j == 3:
            return copy(src, mfwd.at[1], S_MF + 1, ym)
        if other and j == 2:
            return copy(src, mfwd.at[2], S_MF + 2, zm)
        return copy(src, m1.at[me_r], S_M1 + 2 * j + other, (to_z, side, yl, x, h))

    ahead = ((y + 1) % 4) // 2

    def mirror_row_on(slot):
        if slot == 0:
            return copy(mfwd.at[0], m1.at[z * 2 + ahead], S_M1 + 1, ym)
        if slot == 1:
            return copy(mfwd.at[1], m1.at[z * 2 + ahead], S_M1 + 7, (zm[0], *ym[1:]))
        return copy(mfwd.at[2], m1.at[((z + 1) % 4) * 2 + yh], S_M1 + 5, dev(dz=3, dyh=1))

    def mirror_row_in(j, other):
        from_z, from_y = (z + 4 - j) % 4, (yh + other) % 2
        ref = m1.at[from_z * 2 + from_y]
        return copy(ref, ref, S_M1 + 2 * j + other, zp)

    @pl.when(h == 1)
    def _():
        def early(j, carry):
            i = (z + 2 + j) % 4
            product(i)
            out_copy(i).start()
            return carry

        lax.fori_loop(0, 4, early, 0)

    def late(j0, carry):
        j = (j0 + 2) % 4
        i = (z + j) % 4
        product(4 * h + i)

        @pl.when(h == 0)
        def _():
            out_copy(i).wait_recv()
            acc[i] += acc_in[i]

        value = acc[4 * h + i]
        value = value * value
        sums[0, 1] += jnp.sum((value[:, :128] + value[:, 128:]).reshape(32, 8, 128), axis=0)
        for side in range(2):
            for step in range(4):
                for other in range(2):
                    @pl.when(jnp.logical_and(j == step, (yh + other) % 2 == side))
                    def _():
                        if step == 0 and other == 0:
                            m1[me_r] = acc[4 * h + z, :, side * 128:(side + 1) * 128]
                        else:
                            mirror_row(step, side, other).start()

        return carry

    lax.fori_loop(0, 4, late, 0)

    def sum_copies(phase):
        if phase == 0:
            devices = [dev(dx=j // 2, dh=j % 2) for j in range(1, 8)]
        else:
            devices = [dev_zy(j // 4, j % 4) for j in range(1, 16)]
        return [
            copy(sums.at[phase], sums_in.at[7 * phase + j], S_SUM + 7 * phase + j, device)
            for j, device in enumerate(devices)
        ]

    def take_sum(phase):
        copies = sum_copies(phase)
        for c in copies:
            c.wait_recv()
        total = sums[phase]
        for j in range(len(copies)):
            total += sums_in[7 * phase + j]
        return total

    for c in sum_copies(0):
        c.start()

    def send_on(slot):
        copy(mfwd.at[slot], mfwd.at[slot], S_MF + slot, zp).wait_recv()
        mirror_row_on(slot).start()

    send_on(2)
    sums[1] = take_sum(0)
    for c in sum_copies(1):
        c.start()
    send_on(1)
    send_on(0)

    def mirror_col(to_x, to_h):
        index = S_M2 + 2 * ((to_x + 4 - x) % 4) + (to_h + h) % 2
        return copy(m1.at[to_x * 2 + to_h], m2.at[h, x], index, (z, yh, yl, to_x, to_h))

    def mirror_col_in(j):
        from_x, from_h = (x + 4 - j // 2) % 4, (h + j % 2) % 2
        ref = m2.at[from_h, from_x]
        return copy(ref, ref, S_M2 + j, xp)

    for j in (0, 2, 6, 4, 3, 5, 7, 1):
        from_z, from_y = (z + 4 - j // 2) % 4, (yh + j % 2) % 2
        if j > 0:
            mirror_row_in(j // 2, j % 2).wait_recv()
        here = jnp.logical_and(from_z == x, from_y == h)

        @pl.when(here)
        def _():
            m2[h, x] = m1[x * 2 + h]

        @pl.when(jnp.logical_not(here))
        def _():
            mirror_col(from_z, from_y).start()

    load_top.wait()
    total = take_sum(1)
    ratio = jnp.sum(total[1], axis=(0, 1), keepdims=True) / jnp.sum(total[0], axis=(0, 1), keepdims=True)
    balance = jnp.sqrt(jnp.sqrt(ratio))
    half = 0.5 * balance
    inverse = -0.5 / balance

    def finish(j, carry):
        @pl.when(j > 0)
        def _():
            mirror_col_in(j).wait_recv()

        k, xf = (h + j % 2) % 2, (x + 4 - j // 2) % 4
        for m in range(2):
            block = m2[k, xf, m * 128:(m + 1) * 128]
            where = pl.ds(2 * xf + m, 128, stride=8)
            out[k, where, :] = half * top[k, where, :] + inverse * block.T
        return carry

    lax.fori_loop(0, 8, finish, 0)

    for step in range(1, 8):
        for side in range(2):
            below_copy(me_r, side, step, zp).wait_send()
    for side in range(2):
        copy(ball.at[me_r, side], yfwd.at[side], S_FWD + side, yp).wait_send()
    swap_l.wait_send()

    @pl.when(mine_l)
    def _():
        @pl.when(needed(yl, x, z))
        def _():
            for j in range(1, 4):
                l1_copy(j).wait_send()

        def l2_sent(i, xq, zq):
            l2_copy(0, i).wait_send()
            l2_copy(1, i).wait_send()

        l_each(0, yl, l2_sent)
        l_each(3, yl, lambda i, xq, zq: l2_forward(i).wait_send() if i % 2 == 0 else None)
        l_each(1, yl, lambda i, xq, zq: l2_forward(i).wait_send() if i % 2 == 1 else None)

        def ly_sent(i, xq, zq):
            ly_copy(0, xq, zq).wait_send()
            ly_copy(1, xq, zq).wait_send()

        ly_last(yl, ly_sent)

    @pl.when(beside_l)
    def _():
        ly_last(1 - yl, lambda i, xq, zq: ly_copy(2, xq, zq).wait_send())

    def last_y(s, carry):
        y_copy(s).wait_send()
        return carry

    lax.fori_loop(0, 8, last_y, 0)

    @pl.when(h == 1)
    def _():
        for i in range(4):
            out_copy(i).wait_send()

    def last_mirror(j, carry):
        copy(m1.at[0], m1.at[0], S_M1 + j, zp).wait_send()
        copy(m1.at[0], m1.at[0], S_M2 + j, xp).wait_send()
        return carry

    lax.fori_loop(1, 8, last_mirror, 0)
    for slot in range(3):
        copy(mfwd.at[slot], mfwd.at[slot], S_MF + slot, zp).wait_send()
    for phase in range(2):
        for c in sum_copies(phase):
            c.wait_send()


def per_device(matrix, inverse_rest, upper_block, lower_below, lower_inverse):
    vmem = pltpu.VMEM
    dma = pltpu.SemaphoreType.DMA
    result = pl.pallas_call(
        kernel,
        out_shape=jax.ShapeDtypeStruct((2, 1024, 128), F32),
        in_specs=[pl.BlockSpec(memory_space=ANY)] * 5,
        out_specs=pl.BlockSpec(memory_space=pltpu.VMEM),
        scratch_shapes=[
            vmem((8, 2, 7, 128, 128), F32),
            vmem((2, 7, 128, 128), F32),
            vmem((2048, 1792), BF16),
            vmem((256, 2688), BF16),
            vmem((4, 2, 2048, 128), F32),
            vmem((8, 2048, 128), F32),
            vmem((8, 2, 256, 128), F32),
            vmem((8, 2, 512, 128), F32),
            vmem((8, 256, 128), F32),
            vmem((8, 512, 128), F32),
            vmem((2, 8, 256, 128), BF16),
            vmem((2, 2, 4, 4, 128, 256), F32),
            vmem((2, 1024, 256), BF16),
            vmem((8, 256, 256), F32),
            vmem((4, 256, 256), F32),
            vmem((8, 256, 128), F32),
            vmem((2, 4, 256, 128), F32),
            vmem((3, 256, 128), F32),
            vmem((2, 1024, 128), F32),
            vmem((2, 1024, 128), F32),
            vmem((2, 128, 128), F32),
            vmem((2, 128, 128), F32),
            vmem((2, 2, 8, 128), F32),
            vmem((22, 2, 8, 128), F32),
            dma((5,)),
            dma((16,)),
            dma((2,)),
            dma((N_SEM,)),
            dma((N_SEM,)),
        ],
        compiler_params=pltpu.CompilerParams(
            collective_id=0, has_side_effects=True, vmem_limit_bytes=67043328
        ),
    )(
        matrix.reshape(16, 1024, 128),
        inverse_rest.transpose(0, 2, 1, 3).reshape(16, 896, 128),
        upper_block.reshape(2, 128, 128),
        lower_below.transpose(0, 2, 1, 3),
        lower_inverse,
    )
    return result.reshape(2, 128, 8, 128)


def solution(mesh):
    split_mesh = Mesh(mesh.devices.reshape(4, 2, 2, 4, 2), ("row_0", "row_1", "col_0", "col_1", "col_2"))
    return jax.shard_map(
        per_device,
        mesh=split_mesh,
        in_specs=(
            P(None, ROW, None, COL),
            P(None, ROW, None, COL),
            P(None, ROW, None, COL),
            P(None, ROW, None, COL),
            P(None, ROW, COL),
        ),
        out_specs=P(None, ROW, None, COL),
        check_vma=False,
    )
```

```python
import jax
import jax.numpy as jnp
from jax import lax
from jax.experimental import pallas as pl
from jax.experimental.pallas import tpu as pltpu
from jax.sharding import Mesh
from jax.sharding import PartitionSpec as P

ROW = ("row_0", "row_1")
COL = ("col_0", "col_1", "col_2")
MESH = pl.DeviceIdType.MESH
F32 = jnp.float32
BF16 = jnp.bfloat16
ANY = pl.ANY

S_BELOW = 0
S_FWD = 16
S_PAIR = 18
S_A = 50
S_B = 66
S_Y = 82
S_L = 90
S_L2 = 94
S_LY = 106
S_OUT = 154
S_M1 = 158
S_M2 = 166
S_MF = 174
S_SUM = 178
N_SEM = 200


def split(value):
    hi = value.astype(BF16)
    lo = (value - hi.astype(F32)).astype(BF16)
    return hi, lo


def dot_t(a, b):
    return lax.dot_general(a, b, (((1,), (1,)), ((), ())), preferred_element_type=F32)


def dot_n(a, b):
    return lax.dot_general(a, b, (((1,), (0,)), ((), ())), preferred_element_type=F32)


def rows_at(block, count):
    return pl.ds(pl.multiple_of(block * 128, 128), count * 128)


def kernel(
    mat, rest, up, below, linv, out,
    ball, yfwd, rcat, bcat, part, pair, rec_a, rec_b, rec_y, xy, xs, lall, lsplit, acc, acc_in,
    m1, m2, mfwd, top, mstage, ublk, lstage, sums, sums_in,
    in_sem, r_sem, m_sem, send, recv,
):
    z = lax.axis_index("row_0")
    yh = lax.axis_index("row_1")
    yl = lax.axis_index("col_0")
    x = lax.axis_index("col_1")
    h = lax.axis_index("col_2")
    me_r = z * 2 + yh
    y = yh * 2 + yl

    def dev(dz=0, dyh=0, dyl=0, dx=0, dh=0):
        return ((z + dz) % 4, (yh + dyh) % 2, (yl + dyl) % 2, (x + dx) % 4, (h + dh) % 2)

    def dev_y(dy):
        there = (y + dy) % 4
        return (z, there // 2, there % 2, x, h)

    def copy(src, dst, index, device):
        return pltpu.make_async_remote_copy(
            src_ref=src, dst_ref=dst, send_sem=send.at[index], recv_sem=recv.at[index],
            device_id=device, device_id_type=MESH,
        )

    partner = dev(dh=1)
    zp, zm = dev(dz=1), dev(dz=3)
    xp, xm = dev(dx=1), dev(dx=3)
    yp, ym = dev_y(1), dev_y(3)
    ypair = dev(dyl=1)

    load_below = [pltpu.make_async_copy(below.at[k], ball.at[me_r, k], in_sem.at[k]) for k in range(2)]
    load_l = pltpu.make_async_copy(linv, lstage, in_sem.at[2])
    load_u = pltpu.make_async_copy(up, ublk, in_sem.at[3])
    load_top = pltpu.make_async_copy(mat.at[pl.ds(0, 2)], top, in_sem.at[4])

    def staged(p):
        return (p // 4, (p // 2) % 2, pl.ds(pl.multiple_of((p % 2) * 896, 128), 896))

    def load_r(p):
        return pltpu.make_async_copy(rest.at[p], part.at[staged(p)], r_sem.at[p])

    def load_m(p):
        return pltpu.make_async_copy(mat.at[p], mstage.at[p % 2], m_sem.at[p % 2])

    for load in (*load_below, load_l):
        load.start()
    for p in range(16):
        load_r(p).start()
    load_u.start()
    load_top.start()

    barrier = pltpu.get_barrier_semaphore()
    def dev_zy(dz, dy):
        there = (y + dy) % 4
        return ((z + dz) % 4, there // 2, there % 2, x, h)

    friends = [dev_zy(j // 4, j % 4) for j in range(1, 16)]
    friends += [dev(dx=j // 2, dh=j % 2) for j in range(1, 8)]
    for friend in friends:
        pl.semaphore_signal(barrier, inc=1, device_id=friend, device_id_type=MESH)

    sums[...] = jnp.zeros(sums.shape, F32)

    def take_r(p, carry):
        load_r(p).wait()
        where = pl.ds(pl.multiple_of(((p // 4) * 4 + (p % 2) * 2 + (p // 2) % 2) * 128, 128), 128)
        total = jnp.zeros((8, 128), F32)
        for q in range(7):
            rows = pl.ds(pl.multiple_of((p % 2) * 896 + q * 128, 128), 128)
            value = part[p // 4, (p // 2) % 2, rows]
            total += jnp.sum((value * value).reshape(16, 8, 128), axis=0)
            hi, lo = split(value)
            rcat[where, q * 128:(q + 1) * 128] = hi
            rcat[where, (7 + q) * 128:(8 + q) * 128] = lo
        sums[0, 1] += total
        return carry

    lax.fori_loop(0, 8, take_r, 0)
    for load in load_below:
        load.wait()
    load_l.wait()
    pl.semaphore_wait(barrier, len(friends))

    def below_copy(source, half, step, device):
        ref = ball.at[source, half]
        return copy(ref, ref, S_BELOW + 2 * step + half, device)

    below_copy(me_r, 0, 1, zp).start()
    below_copy(me_r, 1, 1, zm).start()
    copy(ball.at[me_r, 0], yfwd.at[0], S_FWD, yp).start()
    copy(ball.at[me_r, 1], yfwd.at[1], S_FWD + 1, ym).start()

    my_l = lall.at[yl, yh, x, z]
    lanes = pl.ds(pl.multiple_of(h * 128, 128), 128)
    swap_l = copy(lstage.at[1 - h], lall.at[yl, yh, x, z, :, lanes], S_L, partner)
    swap_l.start()
    for core in range(2):
        @pl.when(h == core)
        def _():
            lall[yl, yh, x, z, :, core * 128:(core + 1) * 128] = lstage[core]

    lax.fori_loop(8, 16, take_r, 0)
    load_u.wait()

    mine_l = jnp.logical_or(h == 1, yl == 0)
    beside_l = jnp.logical_or(h == 1, yl == 1)
    swap_l.wait_recv()

    def piece_at(i, d):
        return jnp.where(h == 0, (x + d) % 4, i), jnp.where(h == 0, i, (z + d) % 4)

    def dev_first(d):
        return (jnp.where(h == 0, (z + d) % 4, z), yh, yl, jnp.where(h == 0, x, (x + d) % 4), h)

    def dev_second(d):
        return (jnp.where(h == 0, z, (z + d) % 4), yh, yl, jnp.where(h == 0, (x + d) % 4, x), h)

    def needed(yl_from, xq, zq):
        return jnp.logical_or(h != yl_from, xq <= zq)

    def l1_copy(j):
        return copy(my_l, my_l, S_L + j, dev_first(j))

    def l1_wait(j):
        @pl.when(needed(yl, jnp.where(h == 0, x, (x + 4 - j) % 4), jnp.where(h == 0, (z + 4 - j) % 4, z)))
        def _():
            l1_copy(j).wait_recv()

    def l2_copy(side, i):
        xq, zq = piece_at(i, 0)
        ref = lall.at[yl, yh, xq, zq]
        return copy(ref, ref, S_L2 + 4 * side + i, dev_second(1 if side == 0 else 3))

    def l2_forward(i):
        xq, zq = piece_at(i, 3 if i % 2 == 0 else 1)
        ref = lall.at[yl, yh, xq, zq]
        return copy(ref, ref, S_L2 + 8 + i, dev_second(1 if i % 2 == 0 else 3))

    def l_each(d, yl_from, fn):
        for i in range(4):
            xq, zq = piece_at(i, d)

            def one(i=i, xq=xq, zq=zq):
                fn(i, xq, zq)

            pl.when(needed(yl_from, xq, zq))(one)

    def ly_copy(side, xq, zq):
        if side == 2:
            there = (y + jnp.where(yl == 1, 3, 1)) % 4
            target = (y + jnp.where(yl == 1, 1, 3)) % 4
            ref = lall.at[there % 2, there // 2, xq, zq]
            device = (z, target // 2, target % 2, x, h)
        else:
            ref = lall.at[yl, yh, xq, zq]
            device = yp if side == 0 else ym
        return copy(ref, ref, S_LY + 16 * side + xq * 4 + zq, device)

    def ly_wait(side, xq, zq):
        ref = lall.at[yl, yh, xq, zq]
        copy(ref, ref, S_LY + 16 * side + xq * 4 + zq, yp).wait_recv()

    def ly_start(d):
        @pl.when(mine_l)
        def _():
            def fn(i, xq, zq):
                ly_copy(0, xq, zq).start()
                ly_copy(1, xq, zq).start()

            l_each(d, yl, fn)

    def ly_forward(d):
        @pl.when(beside_l)
        def _():
            def fn(i, xq, zq):
                ly_wait(jnp.where(yl == 1, 0, 1), xq, zq)
                ly_copy(2, xq, zq).start()

            l_each(d, 1 - yl, fn)

    @pl.when(jnp.logical_and(mine_l, needed(yl, x, z)))
    def _():
        for j in range(1, 4):
            l1_copy(j).start()

    below_copy(me_r, 1, 2, zp).start()
    below_copy(me_r, 0, 2, zm).start()

    def source(step, half):
        late = jnp.logical_or(step == 3, step >= 5)
        down = jnp.logical_or(step == 1, step == 5)
        up = jnp.logical_or(step == 2, step == 6)
        dz = jnp.where(down, 3 - 2 * half, jnp.where(up, 1 + 2 * half, 0))
        dz = jnp.where(jnp.logical_or(step == 4, step == 7), 2, dz)
        return ((z + dz) % 4) * 2 + (yh + jnp.where(late, 1, 0)) % 2

    def pair_copy(s, share):
        where = rows_at(share * 4, 4)
        return copy(part.at[s % 4, 1 - h, where], pair.at[s, where], S_PAIR + 4 * s + share, partner)

    def add_pair(s, share):
        pair_copy(s, share).wait_recv()

        def add(i, carry):
            where = rows_at(share * 4 + i, 1)
            part[s % 4, h, where] += pair[s, where]
            return carry

        lax.fori_loop(0, 4, add, 0)

    def a_copy(s, side):
        far = (x + 2) % 4
        src = part.at[s % 4, h, rows_at(far * 4 + 2 * side, 2)]
        return copy(src, rec_a.at[s, side], S_A + 2 * s + side, xp if side == 0 else xm)

    def b_copy(s, side):
        near = (x + (1 if side == 0 else 3)) % 4
        src = part.at[s % 4, h, rows_at(near * 4, 4)]
        return copy(src, rec_b.at[s, side], S_B + 2 * s + side, xp if side == 0 else xm)

    def y_copy(s):
        return copy(xy.at[s, rows_at((1 - yl) * 2, 2)], rec_y.at[s], S_Y + s, ypair)

    def step_body(t, carry):
        @pl.when(t < 8)
        def _():
            load_m(2 * t).start()
            load_m(2 * t + 1).start()

        @pl.when(t == 2)
        def _():
            @pl.when(mine_l)
            def _():
                for j in range(1, 4):
                    l1_wait(j)

                def fn(i, xq, zq):
                    l2_copy(0, i).start()
                    l2_copy(1, i).start()

                l_each(0, yl, fn)

            ly_start(0)

        @pl.when(t == 4)
        def _():
            @pl.when(mine_l)
            def _():
                def from_down(i, xq, zq):
                    l2_copy(0, i).wait_recv()
                    if i % 2 == 0:
                        l2_forward(i).start()

                def from_up(i, xq, zq):
                    l2_copy(1, i).wait_recv()
                    if i % 2 == 1:
                        l2_forward(i).start()

                l_each(3, yl, from_down)
                l_each(1, yl, from_up)

            below_copy(source(3, 1), 1, 6, zp).start()
            below_copy(source(3, 0), 0, 6, zm).start()
            ly_start(1)
            ly_start(3)

        @pl.when(t == 5)
        def _():
            ly_forward(0)

        @pl.when(t == 6)
        def _():
            @pl.when(mine_l)
            def _():
                l_each(2, yl, lambda i, xq, zq: l2_forward(i).wait_recv())

            ly_start(2)
            ly_forward(1)

        @pl.when(t == 7)
        def _():
            ly_forward(3)

        @pl.when(t == 8)
        def _():
            ly_forward(2)

        @pl.when(jnp.logical_and(t > 0, t < 8))
        def _():
            for k in range(2):
                below_copy(source(t, k), k, t, zp).wait_recv()

        @pl.when(t == 1)
        def _():
            below_copy(source(1, 0), 0, 4, zp).start()
            below_copy(source(1, 1), 1, 4, zm).start()

        @pl.when(t == 3)
        def _():
            r = source(3, 0)
            below_copy(r, 0, 5, zp).start()
            below_copy(r, 1, 5, zm).start()

        @pl.when(t == 5)
        def _():
            below_copy(source(5, 0), 0, 7, zp).start()
            below_copy(source(5, 1), 1, 7, zm).start()

        @pl.when(t < 8)
        def _():
            for k in range(2):
                for q in range(7):
                    hi, lo = split(ball[source(t, k), k, q])
                    where = slice(k * 128, (k + 1) * 128)
                    bcat[where, q * 128:(q + 1) * 128] = hi
                    bcat[where, (7 + q) * 128:(8 + q) * 128] = hi
                    bcat[where, (14 + q) * 128:(15 + q) * 128] = lo

            def quarter(i, carry):
                share = (x + 2 + i) % 4
                for u in range(2):
                    where = rows_at(share * 4 + 2 * u, 2)
                    value = dot_t(rcat[where, 0:1792], bcat[:, 0:1792]) + dot_t(rcat[where, 0:896], bcat[:, 1792:2688])
                    part[t % 4, 0, where] = value[:, :128]
                    part[t % 4, 1, where] = value[:, 128:]

                @pl.when(jnp.logical_and(x * 2 + h == source(t, yl), share == 0))
                def _():
                    for k in range(2):
                        part[t % 4, yl, k * 256:k * 256 + 128] -= ublk[k]

                pair_copy(t, share).start()
                return carry

            lax.fori_loop(0, 4, quarter, 0)

            for slot in range(2):
                load_m(2 * t + slot).wait()
                value = mstage[slot]
                sums[0, 0] += jnp.sum((value * value).reshape(128, 8, 128), axis=0)

            add_pair(t, (x + 2) % 4)
            a_copy(t, 0).start()
            a_copy(t, 1).start()

        @pl.when(t == 0)
        def _():
            copy(yfwd.at[0], yfwd.at[0], S_FWD, yp).wait_recv()
            copy(yfwd.at[1], yfwd.at[1], S_FWD + 1, ym).wait_recv()
            back = (y + 3) % 4
            copy(yfwd.at[0], ball.at[z * 2 + back // 2, 0], S_BELOW + 6, yp).start()
            ahead = (y + 1) % 4
            copy(yfwd.at[1], ball.at[z * 2 + ahead // 2, 1], S_BELOW + 7, ym).start()

        @pl.when(jnp.logical_and(t >= 1, t < 9))
        def _():
            s = t - 1
            for side in range(2):
                near = (x + (1 if side == 0 else 3)) % 4
                add_pair(s, near)
                a_copy(s, side).wait_recv()
                where = rows_at(near * 4 + 2 * side, 2)
                part[s % 4, h, where] += rec_a[s, side]
                b_copy(s, side).start()
            add_pair(s, x)

        @pl.when(t >= 2)
        def _():
            s = t - 2
            b_copy(s, 0).wait_recv()
            b_copy(s, 1).wait_recv()

            def add(i, carry):
                where = rows_at(i, 1)
                xy[s, where] = part[s % 4, h, rows_at(x * 4 + i, 1)] + rec_b[s, 0, where] + rec_b[s, 1, where]
                return carry

            lax.fori_loop(0, 4, add, 0)
            y_copy(s).start()
            for share in range(4):
                pair_copy(s, share).wait_send()
            for side in range(2):
                a_copy(s, side).wait_send()
                b_copy(s, side).wait_send()

        return carry

    lax.fori_loop(0, 10, step_body, 0)

    def take_y(s, carry):
        y_copy(s).wait_recv()
        hi, lo = split(xy[s, rows_at(yl * 2, 2)] + rec_y[s])
        xs[0, s] = hi
        xs[1, s] = lo
        return carry

    def ly_last(yl_from, fn):
        for d in range(4):
            l_each(d, yl_from, fn)

    def product(i, first, last):
        for s in range(first, last):
            r = source(s, h)
            piece = lall[i // 4, r % 2, i % 4, r // 2]
            hi, lo = split(jnp.where(needed(i // 4, i % 4, r // 2), piece, 0.0))
            lsplit[0, s * 128:(s + 1) * 128] = hi
            lsplit[1, s * 128:(s + 1) * 128] = lo
        rows = slice(first * 128, last * 128)
        left = jnp.concatenate([xs[0, s] for s in range(first, last)], axis=1)
        rest_of = jnp.concatenate([xs[1, s] for s in range(first, last)], axis=1)
        value = dot_n(left, lsplit[0, rows]) + dot_n(rest_of, lsplit[0, rows]) + dot_n(left, lsplit[1, rows])
        if first == 0:
            acc[i] = value
        else:
            acc[i] += value

    def first_part(i, carry):
        product(i, 0, 6)
        return carry

    lax.fori_loop(0, 6, take_y, 0)

    @pl.when(mine_l)
    def _():
        ly_last(yl, lambda i, xq, zq: ly_wait(2, xq, zq))

    @pl.when(beside_l)
    def _():
        ly_last(1 - yl, lambda i, xq, zq: ly_wait(jnp.where(yl == 1, 1, 0), xq, zq))

    lax.fori_loop(0, 4 + 4 * h, first_part, 0)
    lax.fori_loop(6, 8, take_y, 0)

    def out_copy(i):
        return copy(acc.at[i], acc_in.at[i], S_OUT + i, partner)

    def mirror_row(j, side, other):
        to_z = (z + j) % 4
        src = acc.at[4 * h + to_z, :, side * 128:(side + 1) * 128]
        if other and j == 0:
            return copy(src, mfwd.at[0], S_MF, ym)
        if other and j == 3:
            return copy(src, mfwd.at[1], S_MF + 1, ym)
        if other and j == 2:
            return copy(src, mfwd.at[2], S_MF + 2, zm)
        return copy(src, m1.at[me_r], S_M1 + 2 * j + other, (to_z, side, yl, x, h))

    ahead = ((y + 1) % 4) // 2

    def mirror_row_on(slot):
        if slot == 0:
            return copy(mfwd.at[0], m1.at[z * 2 + ahead], S_M1 + 1, ym)
        if slot == 1:
            return copy(mfwd.at[1], m1.at[z * 2 + ahead], S_M1 + 7, (zm[0], *ym[1:]))
        return copy(mfwd.at[2], m1.at[((z + 1) % 4) * 2 + yh], S_M1 + 5, dev(dz=3, dyh=1))

    def mirror_row_in(j, other):
        from_z, from_y = (z + 4 - j) % 4, (yh + other) % 2
        ref = m1.at[from_z * 2 + from_y]
        return copy(ref, ref, S_M1 + 2 * j + other, zp)

    @pl.when(h == 1)
    def _():
        def early(j, carry):
            i = (z + 2 + j) % 4
            product(i, 6, 8)
            out_copy(i).start()
            return carry

        lax.fori_loop(0, 4, early, 0)

    def late(j0, carry):
        j = (j0 + 2) % 4
        i = (z + j) % 4
        product(4 * h + i, 6, 8)

        @pl.when(h == 0)
        def _():
            out_copy(i).wait_recv()
            acc[i] += acc_in[i]

        value = acc[4 * h + i]
        value = value * value
        sums[0, 1] += jnp.sum((value[:, :128] + value[:, 128:]).reshape(32, 8, 128), axis=0)
        for side in range(2):
            for step in range(4):
                for other in range(2):
                    @pl.when(jnp.logical_and(j == step, (yh + other) % 2 == side))
                    def _():
                        if step == 0 and other == 0:
                            m1[me_r] = acc[4 * h + z, :, side * 128:(side + 1) * 128]
                        else:
                            mirror_row(step, side, other).start()

        return carry

    lax.fori_loop(0, 4, late, 0)

    def sum_copies(phase):
        if phase == 0:
            devices = [dev(dx=j // 2, dh=j % 2) for j in range(1, 8)]
        else:
            devices = [dev_zy(j // 4, j % 4) for j in range(1, 16)]
        return [
            copy(sums.at[phase], sums_in.at[7 * phase + j], S_SUM + 7 * phase + j, device)
            for j, device in enumerate(devices)
        ]

    def take_sum(phase):
        copies = sum_copies(phase)
        for c in copies:
            c.wait_recv()
        total = sums[phase]
        for j in range(len(copies)):
            total += sums_in[7 * phase + j]
        return total

    for c in sum_copies(0):
        c.start()

    def mirror_col(to_x, to_h):
        index = S_M2 + 2 * ((to_x + 4 - x) % 4) + (to_h + h) % 2
        return copy(m1.at[to_x * 2 + to_h], m2.at[h, x], index, (z, yh, yl, to_x, to_h))

    def mirror_col_in(j):
        from_x, from_h = (x + 4 - j // 2) % 4, (h + j % 2) % 2
        ref = m2.at[from_h, from_x]
        return copy(ref, ref, S_M2 + j, xp)

    def send_on(slot):
        copy(mfwd.at[slot], mfwd.at[slot], S_MF + slot, zp).wait_recv()
        mirror_row_on(slot).start()

    def spread(j):
        from_z, from_y = (z + 4 - j // 2) % 4, (yh + j % 2) % 2
        if j > 0:
            mirror_row_in(j // 2, j % 2).wait_recv()
        here = jnp.logical_and(from_z == x, from_y == h)

        @pl.when(here)
        def _():
            m2[h, x] = m1[x * 2 + h]

        around = jnp.logical_and(from_z == (x + 2) % 4, j % 2 == 0)

        @pl.when(around)
        def _():
            copy(m1.at[from_z * 2 + from_y], mfwd.at[3], S_MF + 3, xm).start()

        @pl.when(jnp.logical_not(jnp.logical_or(here, around)))
        def _():
            mirror_col(from_z, from_y).start()

    spread(0)
    send_on(2)
    sums[1] = take_sum(0)
    for c in sum_copies(1):
        c.start()
    spread(6)
    send_on(1)
    send_on(0)
    spread(4)
    spread(2)
    copy(mfwd.at[3], mfwd.at[3], S_MF + 3, xm).wait_recv()
    copy(mfwd.at[3], m2.at[h, (x + 1) % 4], S_M2 + 4 + jnp.where(yh == h, 0, 1), (z, yh, yl, (x + 3) % 4, yh)).start()
    for j in (3, 5, 7, 1):
        spread(j)

    load_top.wait()
    total = take_sum(1)
    ratio = jnp.sum(total[1], axis=(0, 1), keepdims=True) / jnp.sum(total[0], axis=(0, 1), keepdims=True)
    balance = jnp.sqrt(jnp.sqrt(ratio))
    half = 0.5 * balance
    inverse = -0.5 / balance

    def finish(j, carry):
        @pl.when(j > 0)
        def _():
            mirror_col_in(j).wait_recv()

        k, xf = (h + j % 2) % 2, (x + 4 - j // 2) % 4
        for m in range(2):
            block = m2[k, xf, m * 128:(m + 1) * 128]
            where = pl.ds(2 * xf + m, 128, stride=8)
            out[k, where, :] = half * top[k, where, :] + inverse * block.T
        return carry

    lax.fori_loop(0, 8, finish, 0)

    for step in range(1, 8):
        for side in range(2):
            below_copy(me_r, side, step, zp).wait_send()
    for side in range(2):
        copy(ball.at[me_r, side], yfwd.at[side], S_FWD + side, yp).wait_send()
    swap_l.wait_send()

    @pl.when(mine_l)
    def _():
        @pl.when(needed(yl, x, z))
        def _():
            for j in range(1, 4):
                l1_copy(j).wait_send()

        def l2_sent(i, xq, zq):
            l2_copy(0, i).wait_send()
            l2_copy(1, i).wait_send()

        l_each(0, yl, l2_sent)
        l_each(3, yl, lambda i, xq, zq: l2_forward(i).wait_send() if i % 2 == 0 else None)
        l_each(1, yl, lambda i, xq, zq: l2_forward(i).wait_send() if i % 2 == 1 else None)

        def ly_sent(i, xq, zq):
            ly_copy(0, xq, zq).wait_send()
            ly_copy(1, xq, zq).wait_send()

        ly_last(yl, ly_sent)

    @pl.when(beside_l)
    def _():
        ly_last(1 - yl, lambda i, xq, zq: ly_copy(2, xq, zq).wait_send())

    def last_y(s, carry):
        y_copy(s).wait_send()
        return carry

    lax.fori_loop(0, 8, last_y, 0)

    @pl.when(h == 1)
    def _():
        for i in range(4):
            out_copy(i).wait_send()

    def last_mirror(j, carry):
        copy(m1.at[0], m1.at[0], S_M1 + j, zp).wait_send()
        copy(m1.at[0], m1.at[0], S_M2 + j, xp).wait_send()
        return carry

    lax.fori_loop(1, 8, last_mirror, 0)
    for slot in range(4):
        copy(mfwd.at[slot], mfwd.at[slot], S_MF + slot, zp).wait_send()
    for phase in range(2):
        for c in sum_copies(phase):
            c.wait_send()


def per_device(matrix, inverse_rest, upper_block, lower_below, lower_inverse):
    vmem = pltpu.VMEM
    dma = pltpu.SemaphoreType.DMA
    result = pl.pallas_call(
        kernel,
        out_shape=jax.ShapeDtypeStruct((2, 1024, 128), F32),
        in_specs=[pl.BlockSpec(memory_space=ANY)] * 5,
        out_specs=pl.BlockSpec(memory_space=pltpu.VMEM),
        scratch_shapes=[
            vmem((8, 2, 7, 128, 128), F32),
            vmem((2, 7, 128, 128), F32),
            vmem((2048, 1792), BF16),
            vmem((256, 2688), BF16),
            vmem((4, 2, 2048, 128), F32),
            vmem((8, 2048, 128), F32),
            vmem((8, 2, 256, 128), F32),
            vmem((8, 2, 512, 128), F32),
            vmem((8, 256, 128), F32),
            vmem((8, 512, 128), F32),
            vmem((2, 8, 256, 128), BF16),
            vmem((2, 2, 4, 4, 128, 256), F32),
            vmem((2, 1024, 256), BF16),
            vmem((8, 256, 256), F32),
            vmem((4, 256, 256), F32),
            vmem((8, 256, 128), F32),
            vmem((2, 4, 256, 128), F32),
            vmem((4, 256, 128), F32),
            vmem((2, 1024, 128), F32),
            vmem((2, 1024, 128), F32),
            vmem((2, 128, 128), F32),
            vmem((2, 128, 128), F32),
            vmem((2, 2, 8, 128), F32),
            vmem((22, 2, 8, 128), F32),
            dma((5,)),
            dma((16,)),
            dma((2,)),
            dma((N_SEM,)),
            dma((N_SEM,)),
        ],
        compiler_params=pltpu.CompilerParams(
            collective_id=0, has_side_effects=True, vmem_limit_bytes=67043328
        ),
    )(
        matrix.reshape(16, 1024, 128),
        inverse_rest.transpose(0, 2, 1, 3).reshape(16, 896, 128),
        upper_block.reshape(2, 128, 128),
        lower_below.transpose(0, 2, 1, 3),
        lower_inverse,
    )
    return result.reshape(2, 128, 8, 128)


def solution(mesh):
    split_mesh = Mesh(mesh.devices.reshape(4, 2, 2, 4, 2), ("row_0", "row_1", "col_0", "col_1", "col_2"))
    return jax.shard_map(
        per_device,
        mesh=split_mesh,
        in_specs=(
            P(None, ROW, None, COL),
            P(None, ROW, None, COL),
            P(None, ROW, None, COL),
            P(None, ROW, None, COL),
            P(None, ROW, COL),
        ),
        out_specs=P(None, ROW, None, COL),
        check_vma=False,
    )
```

```python
import jax
import jax.numpy as jnp
from jax import lax
from jax.experimental import pallas as pl
from jax.experimental.pallas import tpu as pltpu
from jax.sharding import Mesh
from jax.sharding import PartitionSpec as P

ROW = ("row_0", "row_1")
COL = ("col_0", "col_1", "col_2")
MESH = pl.DeviceIdType.MESH
F32 = jnp.float32
BF16 = jnp.bfloat16
ANY = pl.ANY

S_BELOW = 0
S_FWD = 16
S_PAIR = 18
S_A = 50
S_B = 66
S_Y = 82
S_L = 90
S_L2 = 94
S_LY = 106
S_OUT = 154
S_M1 = 158
S_M2 = 166
S_MF = 174
S_SUM = 178
N_SEM = 200


def split(value):
    hi = value.astype(BF16)
    lo = (value - hi.astype(F32)).astype(BF16)
    return hi, lo


def dot_t(a, b):
    return lax.dot_general(a, b, (((1,), (1,)), ((), ())), preferred_element_type=F32)


def dot_n(a, b):
    return lax.dot_general(a, b, (((1,), (0,)), ((), ())), preferred_element_type=F32)


def rows_at(block, count):
    return pl.ds(pl.multiple_of(block * 128, 128), count * 128)


def kernel(
    mat, rest, up, below, linv, out,
    ball, yfwd, rcat, bcat, part, pair, rec_a, rec_b, rec_y, xy, xs, lall, lsplit, acc, acc_in,
    m1, m2, mfwd, top, mstage, ublk, lstage, sums, sums_in,
    in_sem, r_sem, m_sem, send, recv,
):
    z = lax.axis_index("row_0")
    yh = lax.axis_index("row_1")
    yl = lax.axis_index("col_0")
    x = lax.axis_index("col_1")
    h = lax.axis_index("col_2")
    me_r = z * 2 + yh
    y = yh * 2 + yl

    def dev(dz=0, dyh=0, dyl=0, dx=0, dh=0):
        return ((z + dz) % 4, (yh + dyh) % 2, (yl + dyl) % 2, (x + dx) % 4, (h + dh) % 2)

    def dev_y(dy):
        there = (y + dy) % 4
        return (z, there // 2, there % 2, x, h)

    def copy(src, dst, index, device):
        return pltpu.make_async_remote_copy(
            src_ref=src, dst_ref=dst, send_sem=send.at[index], recv_sem=recv.at[index],
            device_id=device, device_id_type=MESH,
        )

    partner = dev(dh=1)
    zp, zm = dev(dz=1), dev(dz=3)
    xp, xm = dev(dx=1), dev(dx=3)
    yp, ym = dev_y(1), dev_y(3)
    ypair = dev(dyl=1)

    load_below = [pltpu.make_async_copy(below.at[k], ball.at[me_r, k], in_sem.at[k]) for k in range(2)]
    load_l = pltpu.make_async_copy(linv, lstage, in_sem.at[2])
    load_u = pltpu.make_async_copy(up, ublk, in_sem.at[3])
    load_top = pltpu.make_async_copy(mat.at[pl.ds(0, 2)], top, in_sem.at[4])

    def staged(p):
        return (p // 4, (p // 2) % 2, pl.ds(pl.multiple_of((p % 2) * 896, 128), 896))

    def load_r(p):
        return pltpu.make_async_copy(rest.at[p], part.at[staged(p)], r_sem.at[p])

    def load_m(p):
        return pltpu.make_async_copy(mat.at[p], mstage.at[p % 2], m_sem.at[p % 2])

    for load in (*load_below, load_l):
        load.start()
    for p in range(16):
        load_r(p).start()
    load_u.start()
    load_top.start()

    barrier = pltpu.get_barrier_semaphore()
    def dev_zy(dz, dy):
        there = (y + dy) % 4
        return ((z + dz) % 4, there // 2, there % 2, x, h)

    friends = [dev_zy(j // 4, j % 4) for j in range(1, 16)]
    friends += [dev(dx=j // 2, dh=j % 2) for j in range(1, 8)]
    for friend in friends:
        pl.semaphore_signal(barrier, inc=1, device_id=friend, device_id_type=MESH)

    sums[...] = jnp.zeros(sums.shape, F32)

    def take_r(p, carry):
        load_r(p).wait()
        where = pl.ds(pl.multiple_of(((p // 4) * 4 + (p % 2) * 2 + (p // 2) % 2) * 128, 128), 128)
        total = jnp.zeros((8, 128), F32)
        for q in range(7):
            rows = pl.ds(pl.multiple_of((p % 2) * 896 + q * 128, 128), 128)
            value = part[p // 4, (p // 2) % 2, rows]
            total += jnp.sum((value * value).reshape(16, 8, 128), axis=0)
            hi, lo = split(value)
            rcat[where, q * 128:(q + 1) * 128] = hi
            rcat[where, (7 + q) * 128:(8 + q) * 128] = lo
        sums[0, 1] += total
        return carry

    lax.fori_loop(0, 8, take_r, 0)
    for load in load_below:
        load.wait()
    load_l.wait()
    pl.semaphore_wait(barrier, len(friends))

    def below_copy(source, half, step, device):
        ref = ball.at[source, half]
        return copy(ref, ref, S_BELOW + 2 * step + half, device)

    below_copy(me_r, 0, 1, zp).start()
    below_copy(me_r, 1, 1, zm).start()
    copy(ball.at[me_r, 0], yfwd.at[0], S_FWD, yp).start()
    copy(ball.at[me_r, 1], yfwd.at[1], S_FWD + 1, ym).start()

    my_l = lall.at[yl, yh, x, z]
    lanes = pl.ds(pl.multiple_of(h * 128, 128), 128)
    swap_l = copy(lstage.at[1 - h], lall.at[yl, yh, x, z, :, lanes], S_L, partner)
    swap_l.start()
    for core in range(2):
        @pl.when(h == core)
        def _():
            lall[yl, yh, x, z, :, core * 128:(core + 1) * 128] = lstage[core]

    lax.fori_loop(8, 16, take_r, 0)
    load_u.wait()

    mine_l = jnp.logical_or(h == 1, yl == 0)
    beside_l = jnp.logical_or(h == 1, yl == 1)
    swap_l.wait_recv()

    def piece_at(i, d):
        return jnp.where(h == 0, (x + d) % 4, i), jnp.where(h == 0, i, (z + d) % 4)

    def dev_first(d):
        return (jnp.where(h == 0, (z + d) % 4, z), yh, yl, jnp.where(h == 0, x, (x + d) % 4), h)

    def dev_second(d):
        return (jnp.where(h == 0, z, (z + d) % 4), yh, yl, jnp.where(h == 0, (x + d) % 4, x), h)

    def needed(yl_from, xq, zq):
        return jnp.logical_or(h != yl_from, xq <= zq)

    def l1_copy(j):
        return copy(my_l, my_l, S_L + j, dev_first(j))

    def l1_wait(j):
        @pl.when(needed(yl, jnp.where(h == 0, x, (x + 4 - j) % 4), jnp.where(h == 0, (z + 4 - j) % 4, z)))
        def _():
            l1_copy(j).wait_recv()

    def l2_copy(side, i):
        xq, zq = piece_at(i, 0)
        ref = lall.at[yl, yh, xq, zq]
        return copy(ref, ref, S_L2 + 4 * side + i, dev_second(1 if side == 0 else 3))

    def l2_forward(i):
        xq, zq = piece_at(i, 3 if i % 2 == 0 else 1)
        ref = lall.at[yl, yh, xq, zq]
        return copy(ref, ref, S_L2 + 8 + i, dev_second(1 if i % 2 == 0 else 3))

    def l_each(d, yl_from, fn):
        for i in range(4):
            xq, zq = piece_at(i, d)

            def one(i=i, xq=xq, zq=zq):
                fn(i, xq, zq)

            pl.when(needed(yl_from, xq, zq))(one)

    def ly_copy(side, xq, zq):
        if side == 2:
            there = (y + jnp.where(yl == 1, 3, 1)) % 4
            target = (y + jnp.where(yl == 1, 1, 3)) % 4
            ref = lall.at[there % 2, there // 2, xq, zq]
            device = (z, target // 2, target % 2, x, h)
        else:
            ref = lall.at[yl, yh, xq, zq]
            device = yp if side == 0 else ym
        return copy(ref, ref, S_LY + 16 * side + xq * 4 + zq, device)

    def ly_wait(side, xq, zq):
        ref = lall.at[yl, yh, xq, zq]
        copy(ref, ref, S_LY + 16 * side + xq * 4 + zq, yp).wait_recv()

    def ly_start(d):
        @pl.when(mine_l)
        def _():
            def fn(i, xq, zq):
                ly_copy(0, xq, zq).start()
                ly_copy(1, xq, zq).start()

            l_each(d, yl, fn)

    def ly_forward(d):
        @pl.when(beside_l)
        def _():
            def fn(i, xq, zq):
                ly_wait(jnp.where(yl == 1, 0, 1), xq, zq)
                ly_copy(2, xq, zq).start()

            l_each(d, 1 - yl, fn)

    @pl.when(jnp.logical_and(mine_l, needed(yl, x, z)))
    def _():
        for j in range(1, 4):
            l1_copy(j).start()

    below_copy(me_r, 1, 2, zp).start()
    below_copy(me_r, 0, 2, zm).start()

    def source(step, half):
        late = jnp.logical_or(step == 3, step >= 5)
        down = jnp.logical_or(step == 1, step == 5)
        up = jnp.logical_or(step == 2, step == 6)
        dz = jnp.where(down, 3 - 2 * half, jnp.where(up, 1 + 2 * half, 0))
        dz = jnp.where(jnp.logical_or(step == 4, step == 7), 2, dz)
        return ((z + dz) % 4) * 2 + (yh + jnp.where(late, 1, 0)) % 2

    def pair_copy(s, share):
        where = rows_at(share * 4, 4)
        return copy(part.at[s % 4, 1 - h, where], pair.at[s, where], S_PAIR + 4 * s + share, partner)

    def add_pair(s, share):
        pair_copy(s, share).wait_recv()

        def add(i, carry):
            where = rows_at(share * 4 + i, 1)
            part[s % 4, h, where] += pair[s, where]
            return carry

        lax.fori_loop(0, 4, add, 0)

    def a_copy(s, side):
        far = (x + 2) % 4
        src = part.at[s % 4, h, rows_at(far * 4 + 2 * side, 2)]
        return copy(src, rec_a.at[s, side], S_A + 2 * s + side, xp if side == 0 else xm)

    def b_copy(s, side):
        near = (x + (1 if side == 0 else 3)) % 4
        src = part.at[s % 4, h, rows_at(near * 4, 4)]
        return copy(src, rec_b.at[s, side], S_B + 2 * s + side, xp if side == 0 else xm)

    def y_copy(s):
        return copy(xy.at[s, rows_at((1 - yl) * 2, 2)], rec_y.at[s], S_Y + s, ypair)

    def step_body(t, carry):
        @pl.when(t < 8)
        def _():
            load_m(2 * t).start()
            load_m(2 * t + 1).start()

        @pl.when(t == 2)
        def _():
            @pl.when(mine_l)
            def _():
                for j in range(1, 4):
                    l1_wait(j)

                def fn(i, xq, zq):
                    l2_copy(0, i).start()
                    l2_copy(1, i).start()

                l_each(0, yl, fn)

            ly_start(0)

        def second_halves():
            below_copy(source(3, 1), 1, 6, zp).start()
            below_copy(source(3, 0), 0, 6, zm).start()

        @pl.when(t == 4)
        def _():
            pl.when(h == 0)(second_halves)

            @pl.when(mine_l)
            def _():
                def from_down(i, xq, zq):
                    l2_copy(0, i).wait_recv()
                    if i % 2 == 0:
                        l2_forward(i).start()

                def from_up(i, xq, zq):
                    l2_copy(1, i).wait_recv()
                    if i % 2 == 1:
                        l2_forward(i).start()

                l_each(3, yl, from_down)
                l_each(1, yl, from_up)

            pl.when(h == 1)(second_halves)
            ly_start(1)
            ly_start(3)

        @pl.when(t == 5)
        def _():
            ly_forward(0)

        @pl.when(t == 6)
        def _():
            @pl.when(mine_l)
            def _():
                l_each(2, yl, lambda i, xq, zq: l2_forward(i).wait_recv())

            ly_start(2)
            ly_forward(1)

        @pl.when(t == 7)
        def _():
            ly_forward(3)

        @pl.when(t == 8)
        def _():
            ly_forward(2)

        @pl.when(jnp.logical_and(t > 0, t < 8))
        def _():
            for k in range(2):
                below_copy(source(t, k), k, t, zp).wait_recv()

        @pl.when(t == 1)
        def _():
            below_copy(source(1, 0), 0, 4, zp).start()
            below_copy(source(1, 1), 1, 4, zm).start()

        @pl.when(t == 3)
        def _():
            r = source(3, 0)
            below_copy(r, 0, 5, zp).start()
            below_copy(r, 1, 5, zm).start()

        @pl.when(t == 5)
        def _():
            below_copy(source(5, 0), 0, 7, zp).start()
            below_copy(source(5, 1), 1, 7, zm).start()

        @pl.when(t < 8)
        def _():
            for k in range(2):
                for q in range(7):
                    hi, lo = split(ball[source(t, k), k, q])
                    where = slice(k * 128, (k + 1) * 128)
                    bcat[where, q * 128:(q + 1) * 128] = hi
                    bcat[where, (7 + q) * 128:(8 + q) * 128] = hi
                    bcat[where, (14 + q) * 128:(15 + q) * 128] = lo

            def quarter(i, carry):
                share = (x + 2 + i) % 4
                for u in range(2):
                    where = rows_at(share * 4 + 2 * u, 2)
                    value = dot_t(rcat[where, 0:1792], bcat[:, 0:1792]) + dot_t(rcat[where, 0:896], bcat[:, 1792:2688])
                    part[t % 4, 0, where] = value[:, :128]
                    part[t % 4, 1, where] = value[:, 128:]

                @pl.when(jnp.logical_and(x * 2 + h == source(t, yl), share == 0))
                def _():
                    for k in range(2):
                        part[t % 4, yl, k * 256:k * 256 + 128] -= ublk[k]

                pair_copy(t, share).start()
                return carry

            lax.fori_loop(0, 4, quarter, 0)

            for slot in range(2):
                load_m(2 * t + slot).wait()
                value = mstage[slot]
                sums[0, 0] += jnp.sum((value * value).reshape(128, 8, 128), axis=0)

            add_pair(t, (x + 2) % 4)
            a_copy(t, 0).start()
            a_copy(t, 1).start()

        @pl.when(t == 0)
        def _():
            copy(yfwd.at[0], yfwd.at[0], S_FWD, yp).wait_recv()
            copy(yfwd.at[1], yfwd.at[1], S_FWD + 1, ym).wait_recv()
            back = (y + 3) % 4
            copy(yfwd.at[0], ball.at[z * 2 + back // 2, 0], S_BELOW + 6, yp).start()
            ahead = (y + 1) % 4
            copy(yfwd.at[1], ball.at[z * 2 + ahead // 2, 1], S_BELOW + 7, ym).start()

        @pl.when(jnp.logical_and(t >= 1, t < 9))
        def _():
            s = t - 1
            for side in range(2):
                near = (x + (1 if side == 0 else 3)) % 4
                add_pair(s, near)
                a_copy(s, side).wait_recv()
                where = rows_at(near * 4 + 2 * side, 2)
                part[s % 4, h, where] += rec_a[s, side]
                b_copy(s, side).start()
            add_pair(s, x)

        @pl.when(t >= 2)
        def _():
            s = t - 2
            b_copy(s, 0).wait_recv()
            b_copy(s, 1).wait_recv()

            def add(i, carry):
                where = rows_at(i, 1)
                xy[s, where] = part[s % 4, h, rows_at(x * 4 + i, 1)] + rec_b[s, 0, where] + rec_b[s, 1, where]
                return carry

            lax.fori_loop(0, 4, add, 0)
            y_copy(s).start()
            for share in range(4):
                pair_copy(s, share).wait_send()
            for side in range(2):
                a_copy(s, side).wait_send()
                b_copy(s, side).wait_send()

        return carry

    lax.fori_loop(0, 10, step_body, 0)

    def take_y(s, carry):
        y_copy(s).wait_recv()
        hi, lo = split(xy[s, rows_at(yl * 2, 2)] + rec_y[s])
        xs[0, s] = hi
        xs[1, s] = lo
        return carry

    def ly_last(yl_from, fn):
        for d in range(4):
            l_each(d, yl_from, fn)

    def product(i, first, last):
        for s in range(first, last):
            r = source(s, h)
            piece = lall[i // 4, r % 2, i % 4, r // 2]
            hi, lo = split(jnp.where(needed(i // 4, i % 4, r // 2), piece, 0.0))
            lsplit[0, s * 128:(s + 1) * 128] = hi
            lsplit[1, s * 128:(s + 1) * 128] = lo
        rows = slice(first * 128, last * 128)
        left = jnp.concatenate([xs[0, s] for s in range(first, last)], axis=1)
        rest_of = jnp.concatenate([xs[1, s] for s in range(first, last)], axis=1)
        value = dot_n(left, lsplit[0, rows]) + dot_n(rest_of, lsplit[0, rows]) + dot_n(left, lsplit[1, rows])
        if first == 0:
            acc[i] = value
        else:
            acc[i] += value

    def first_part(i, carry):
        product(i, 0, 6)
        return carry

    lax.fori_loop(0, 6, take_y, 0)

    @pl.when(mine_l)
    def _():
        ly_last(yl, lambda i, xq, zq: ly_wait(2, xq, zq))

    @pl.when(beside_l)
    def _():
        ly_last(1 - yl, lambda i, xq, zq: ly_wait(jnp.where(yl == 1, 1, 0), xq, zq))

    lax.fori_loop(0, 4 + 4 * h, first_part, 0)
    lax.fori_loop(6, 8, take_y, 0)

    def out_copy(i):
        return copy(acc.at[i], acc_in.at[i], S_OUT + i, partner)

    def mirror_row(j, side, other):
        to_z = (z + j) % 4
        src = acc.at[4 * h + to_z, :, side * 128:(side + 1) * 128]
        if other and j == 0:
            return copy(src, mfwd.at[0], S_MF, ym)
        if other and j == 3:
            return copy(src, mfwd.at[1], S_MF + 1, ym)
        if other and j == 2:
            return copy(src, mfwd.at[2], S_MF + 2, zm)
        return copy(src, m1.at[me_r], S_M1 + 2 * j + other, (to_z, side, yl, x, h))

    ahead = ((y + 1) % 4) // 2

    def mirror_row_on(slot):
        if slot == 0:
            return copy(mfwd.at[0], m1.at[z * 2 + ahead], S_M1 + 1, ym)
        if slot == 1:
            return copy(mfwd.at[1], m1.at[z * 2 + ahead], S_M1 + 7, (zm[0], *ym[1:]))
        return copy(mfwd.at[2], m1.at[((z + 1) % 4) * 2 + yh], S_M1 + 5, dev(dz=3, dyh=1))

    def mirror_row_in(j, other):
        from_z, from_y = (z + 4 - j) % 4, (yh + other) % 2
        ref = m1.at[from_z * 2 + from_y]
        return copy(ref, ref, S_M1 + 2 * j + other, zp)

    @pl.when(h == 1)
    def _():
        def early(j, carry):
            i = (z + 2 + j) % 4
            product(i, 6, 8)
            out_copy(i).start()
            return carry

        lax.fori_loop(0, 4, early, 0)

    def late(j0, carry):
        j = (j0 + 2) % 4
        i = (z + j) % 4
        product(4 * h + i, 6, 8)

        @pl.when(h == 0)
        def _():
            out_copy(i).wait_recv()
            acc[i] += acc_in[i]

        for side in range(2):
            for step in range(4):
                for other in range(2):
                    @pl.when(jnp.logical_and(j == step, (yh + other) % 2 == side))
                    def _():
                        if step == 0 and other == 0:
                            m1[me_r] = acc[4 * h + z, :, side * 128:(side + 1) * 128]
                        else:
                            mirror_row(step, side, other).start()

        value = acc[4 * h + i]
        value = value * value
        sums[0, 1] += jnp.sum((value[:, :128] + value[:, 128:]).reshape(32, 8, 128), axis=0)
        return carry

    lax.fori_loop(0, 4, late, 0)

    def sum_copies(phase):
        if phase == 0:
            devices = [dev(dx=j // 2, dh=j % 2) for j in range(1, 8)]
        else:
            devices = [dev_zy(j // 4, j % 4) for j in range(1, 16)]
        return [
            copy(sums.at[phase], sums_in.at[7 * phase + j], S_SUM + 7 * phase + j, device)
            for j, device in enumerate(devices)
        ]

    def take_sum(phase):
        copies = sum_copies(phase)
        for c in copies:
            c.wait_recv()
        total = sums[phase]
        for j in range(len(copies)):
            total += sums_in[7 * phase + j]
        return total

    for c in sum_copies(0):
        c.start()

    def mirror_col(to_x, to_h):
        index = S_M2 + 2 * ((to_x + 4 - x) % 4) + (to_h + h) % 2
        return copy(m1.at[to_x * 2 + to_h], m2.at[h, x], index, (z, yh, yl, to_x, to_h))

    def mirror_col_in(j):
        from_x, from_h = (x + 4 - j // 2) % 4, (h + j % 2) % 2
        ref = m2.at[from_h, from_x]
        return copy(ref, ref, S_M2 + j, xp)

    def send_on(slot):
        copy(mfwd.at[slot], mfwd.at[slot], S_MF + slot, zp).wait_recv()
        mirror_row_on(slot).start()

    def spread(j):
        from_z, from_y = (z + 4 - j // 2) % 4, (yh + j % 2) % 2
        if j > 0:
            mirror_row_in(j // 2, j % 2).wait_recv()
        here = jnp.logical_and(from_z == x, from_y == h)

        @pl.when(here)
        def _():
            m2[h, x] = m1[x * 2 + h]

        around = jnp.logical_and(from_z == (x + 2) % 4, j % 2 == 0)

        @pl.when(around)
        def _():
            copy(m1.at[from_z * 2 + from_y], mfwd.at[3], S_MF + 3, xm).start()

        @pl.when(jnp.logical_not(jnp.logical_or(here, around)))
        def _():
            mirror_col(from_z, from_y).start()

    spread(0)
    send_on(2)
    sums[1] = take_sum(0)
    for c in sum_copies(1):
        c.start()
    spread(6)
    send_on(1)
    send_on(0)
    spread(4)
    spread(2)
    copy(mfwd.at[3], mfwd.at[3], S_MF + 3, xm).wait_recv()
    copy(mfwd.at[3], m2.at[h, (x + 1) % 4], S_M2 + 4 + jnp.where(yh == h, 0, 1), (z, yh, yl, (x + 3) % 4, yh)).start()
    for j in (3, 5, 7, 1):
        spread(j)

    load_top.wait()
    total = take_sum(1)
    ratio = jnp.sum(total[1], axis=(0, 1), keepdims=True) / jnp.sum(total[0], axis=(0, 1), keepdims=True)
    balance = jnp.sqrt(jnp.sqrt(ratio))
    half = 0.5 * balance
    inverse = -0.5 / balance

    def finish(j, carry):
        @pl.when(j > 0)
        def _():
            mirror_col_in(j).wait_recv()

        k, xf = (h + j % 2) % 2, (x + 4 - j // 2) % 4
        for m in range(2):
            block = m2[k, xf, m * 128:(m + 1) * 128]
            where = pl.ds(2 * xf + m, 128, stride=8)
            out[k, where, :] = half * top[k, where, :] + inverse * block.T
        return carry

    lax.fori_loop(0, 8, finish, 0)

    for step in range(1, 8):
        for side in range(2):
            below_copy(me_r, side, step, zp).wait_send()
    for side in range(2):
        copy(ball.at[me_r, side], yfwd.at[side], S_FWD + side, yp).wait_send()
    swap_l.wait_send()

    @pl.when(mine_l)
    def _():
        @pl.when(needed(yl, x, z))
        def _():
            for j in range(1, 4):
                l1_copy(j).wait_send()

        def l2_sent(i, xq, zq):
            l2_copy(0, i).wait_send()
            l2_copy(1, i).wait_send()

        l_each(0, yl, l2_sent)
        l_each(3, yl, lambda i, xq, zq: l2_forward(i).wait_send() if i % 2 == 0 else None)
        l_each(1, yl, lambda i, xq, zq: l2_forward(i).wait_send() if i % 2 == 1 else None)

        def ly_sent(i, xq, zq):
            ly_copy(0, xq, zq).wait_send()
            ly_copy(1, xq, zq).wait_send()

        ly_last(yl, ly_sent)

    @pl.when(beside_l)
    def _():
        ly_last(1 - yl, lambda i, xq, zq: ly_copy(2, xq, zq).wait_send())

    def last_y(s, carry):
        y_copy(s).wait_send()
        return carry

    lax.fori_loop(0, 8, last_y, 0)

    @pl.when(h == 1)
    def _():
        for i in range(4):
            out_copy(i).wait_send()

    def last_mirror(j, carry):
        copy(m1.at[0], m1.at[0], S_M1 + j, zp).wait_send()
        copy(m1.at[0], m1.at[0], S_M2 + j, xp).wait_send()
        return carry

    lax.fori_loop(1, 8, last_mirror, 0)
    for slot in range(4):
        copy(mfwd.at[slot], mfwd.at[slot], S_MF + slot, zp).wait_send()
    for phase in range(2):
        for c in sum_copies(phase):
            c.wait_send()


def per_device(matrix, inverse_rest, upper_block, lower_below, lower_inverse):
    vmem = pltpu.VMEM
    dma = pltpu.SemaphoreType.DMA
    result = pl.pallas_call(
        kernel,
        out_shape=pltpu.VMEM((2, 1024, 128), F32),
        in_specs=[pl.BlockSpec(memory_space=ANY)] * 5,
        out_specs=pl.BlockSpec(memory_space=pltpu.VMEM),
        scratch_shapes=[
            vmem((8, 2, 7, 128, 128), F32),
            vmem((2, 7, 128, 128), F32),
            vmem((2048, 1792), BF16),
            vmem((256, 2688), BF16),
            vmem((4, 2, 2048, 128), F32),
            vmem((8, 2048, 128), F32),
            vmem((8, 2, 256, 128), F32),
            vmem((8, 2, 512, 128), F32),
            vmem((8, 256, 128), F32),
            vmem((8, 512, 128), F32),
            vmem((2, 8, 256, 128), BF16),
            vmem((2, 2, 4, 4, 128, 256), F32),
            vmem((2, 1024, 256), BF16),
            vmem((8, 256, 256), F32),
            vmem((4, 256, 256), F32),
            vmem((8, 256, 128), F32),
            vmem((2, 4, 256, 128), F32),
            vmem((4, 256, 128), F32),
            vmem((2, 1024, 128), F32),
            vmem((2, 1024, 128), F32),
            vmem((2, 128, 128), F32),
            vmem((2, 128, 128), F32),
            vmem((2, 2, 8, 128), F32),
            vmem((22, 2, 8, 128), F32),
            dma((5,)),
            dma((16,)),
            dma((2,)),
            dma((N_SEM,)),
            dma((N_SEM,)),
        ],
        compiler_params=pltpu.CompilerParams(
            collective_id=0, has_side_effects=True, vmem_limit_bytes=64500000
        ),
    )(
        matrix.reshape(16, 1024, 128),
        inverse_rest.transpose(0, 2, 1, 3).reshape(16, 896, 128),
        upper_block.reshape(2, 128, 128),
        lower_below.transpose(0, 2, 1, 3),
        lower_inverse,
    )
    return result.reshape(2, 128, 8, 128)


def solution(mesh):
    split_mesh = Mesh(mesh.devices.reshape(4, 2, 2, 4, 2), ("row_0", "row_1", "col_0", "col_1", "col_2"))
    return jax.shard_map(
        per_device,
        mesh=split_mesh,
        in_specs=(
            P(None, ROW, None, COL),
            P(None, ROW, None, COL),
            P(None, ROW, None, COL),
            P(None, ROW, None, COL),
            P(None, ROW, COL),
        ),
        out_specs=P(None, ROW, None, COL),
        check_vma=False,
    )
```

```python
import jax
import jax.numpy as jnp
from jax import lax
from jax.experimental import pallas as pl
from jax.experimental.pallas import tpu as pltpu
from jax.sharding import Mesh
from jax.sharding import PartitionSpec as P

ROW = ("row_0", "row_1")
COL = ("col_0", "col_1", "col_2")
MESH = pl.DeviceIdType.MESH
F32 = jnp.float32
BF16 = jnp.bfloat16
ANY = pl.ANY

S_BELOW = 0
S_FWD = 16
S_PAIR = 18
S_A = 50
S_B = 66
S_Y = 82
S_L = 90
S_L2 = 94
S_LY = 106
S_OUT = 154
S_M1 = 158
S_M2 = 166
S_MF = 174
S_SUM = 178
N_SEM = 200


def split(value):
    hi = value.astype(BF16)
    lo = (value - hi.astype(F32)).astype(BF16)
    return hi, lo


def dot_t(a, b):
    return lax.dot_general(a, b, (((1,), (1,)), ((), ())), preferred_element_type=F32)


def dot_n(a, b):
    return lax.dot_general(a, b, (((1,), (0,)), ((), ())), preferred_element_type=F32)


def rows_at(block, count):
    return pl.ds(pl.multiple_of(block * 128, 128), count * 128)


def kernel(
    mat, rest, up, below, linv, out,
    ball, yfwd, rcat, bcat, part, pair, rec_a, rec_b, rec_y, xy, xs, lall, lsplit, acc, acc_in,
    m1, m2, mfwd, top, mstage, ublk, lstage, sums, sums_in,
    in_sem, r_sem, m_sem, send, recv,
):
    z = lax.axis_index("row_0")
    yh = lax.axis_index("row_1")
    yl = lax.axis_index("col_0")
    x = lax.axis_index("col_1")
    h = lax.axis_index("col_2")
    me_r = z * 2 + yh
    y = yh * 2 + yl

    def dev(dz=0, dyh=0, dyl=0, dx=0, dh=0):
        return ((z + dz) % 4, (yh + dyh) % 2, (yl + dyl) % 2, (x + dx) % 4, (h + dh) % 2)

    def dev_y(dy):
        there = (y + dy) % 4
        return (z, there // 2, there % 2, x, h)

    def copy(src, dst, index, device):
        return pltpu.make_async_remote_copy(
            src_ref=src, dst_ref=dst, send_sem=send.at[index], recv_sem=recv.at[index],
            device_id=device, device_id_type=MESH,
        )

    partner = dev(dh=1)
    zp, zm = dev(dz=1), dev(dz=3)
    xp, xm = dev(dx=1), dev(dx=3)
    yp, ym = dev_y(1), dev_y(3)
    ypair = dev(dyl=1)

    load_below = [pltpu.make_async_copy(below.at[k], ball.at[me_r, k], in_sem.at[k]) for k in range(2)]
    load_l = pltpu.make_async_copy(linv, lstage, in_sem.at[2])
    load_u = pltpu.make_async_copy(up, ublk, in_sem.at[3])
    load_top = pltpu.make_async_copy(mat.at[pl.ds(0, 2)], top, in_sem.at[4])

    def staged(p):
        return (p // 4, (p // 2) % 2, pl.ds(pl.multiple_of((p % 2) * 896, 128), 896))

    def load_r(p):
        return pltpu.make_async_copy(rest.at[p], part.at[staged(p)], r_sem.at[p])

    def load_m(p):
        return pltpu.make_async_copy(mat.at[p], mstage.at[p % 2], m_sem.at[p % 2])

    for load in (*load_below, load_l):
        load.start()
    for p in range(16):
        load_r(p).start()
    load_u.start()
    load_top.start()

    barrier = pltpu.get_barrier_semaphore()
    def dev_zy(dz, dy):
        there = (y + dy) % 4
        return ((z + dz) % 4, there // 2, there % 2, x, h)

    friends = [dev_zy(j // 4, j % 4) for j in range(1, 16)]
    friends += [dev(dx=j // 2, dh=j % 2) for j in range(1, 8)]
    for friend in friends:
        pl.semaphore_signal(barrier, inc=1, device_id=friend, device_id_type=MESH)

    sums[...] = jnp.zeros(sums.shape, F32)

    def take_r(p, carry):
        load_r(p).wait()
        where = pl.ds(pl.multiple_of(((p // 4) * 4 + (p % 2) * 2 + (p // 2) % 2) * 128, 128), 128)
        total = jnp.zeros((8, 128), F32)
        for q in range(7):
            rows = pl.ds(pl.multiple_of((p % 2) * 896 + q * 128, 128), 128)
            value = part[p // 4, (p // 2) % 2, rows]
            total += jnp.sum((value * value).reshape(16, 8, 128), axis=0)
            hi, lo = split(value)
            rcat[where, q * 128:(q + 1) * 128] = hi
            rcat[where, (7 + q) * 128:(8 + q) * 128] = lo
        sums[0, 1] += total
        return carry

    lax.fori_loop(0, 8, take_r, 0)
    for load in load_below:
        load.wait()
    load_l.wait()
    pl.semaphore_wait(barrier, len(friends))

    def below_copy(source, half, step, device):
        ref = ball.at[source, half]
        return copy(ref, ref, S_BELOW + 2 * step + half, device)

    below_copy(me_r, 0, 1, zp).start()
    below_copy(me_r, 1, 1, zm).start()
    copy(ball.at[me_r, 0], yfwd.at[0], S_FWD, yp).start()
    copy(ball.at[me_r, 1], yfwd.at[1], S_FWD + 1, ym).start()

    my_l = lall.at[yl, yh, x, z]
    lanes = pl.ds(pl.multiple_of(h * 128, 128), 128)
    swap_l = copy(lstage.at[1 - h], lall.at[yl, yh, x, z, :, lanes], S_L, partner)
    swap_l.start()
    for core in range(2):
        @pl.when(h == core)
        def _():
            lall[yl, yh, x, z, :, core * 128:(core + 1) * 128] = lstage[core]

    lax.fori_loop(8, 16, take_r, 0)
    load_u.wait()

    mine_l = jnp.logical_or(h == 1, yl == 0)
    beside_l = jnp.logical_or(h == 1, yl == 1)
    swap_l.wait_recv()

    def piece_at(i, d):
        return jnp.where(h == 0, (x + d) % 4, i), jnp.where(h == 0, i, (z + d) % 4)

    def dev_first(d):
        return (jnp.where(h == 0, (z + d) % 4, z), yh, yl, jnp.where(h == 0, x, (x + d) % 4), h)

    def dev_second(d):
        return (jnp.where(h == 0, z, (z + d) % 4), yh, yl, jnp.where(h == 0, (x + d) % 4, x), h)

    def needed(yl_from, xq, zq):
        return jnp.logical_or(h != yl_from, xq <= zq)

    def l1_copy(j):
        return copy(my_l, my_l, S_L + j, dev_first(j))

    def l1_wait(j):
        @pl.when(needed(yl, jnp.where(h == 0, x, (x + 4 - j) % 4), jnp.where(h == 0, (z + 4 - j) % 4, z)))
        def _():
            l1_copy(j).wait_recv()

    def l2_copy(side, i):
        xq, zq = piece_at(i, 0)
        ref = lall.at[yl, yh, xq, zq]
        return copy(ref, ref, S_L2 + 4 * side + i, dev_second(1 if side == 0 else 3))

    def l2_forward(i):
        xq, zq = piece_at(i, 3 if i % 2 == 0 else 1)
        ref = lall.at[yl, yh, xq, zq]
        return copy(ref, ref, S_L2 + 8 + i, dev_second(1 if i % 2 == 0 else 3))

    def l_each(d, yl_from, fn):
        for i in range(4):
            xq, zq = piece_at(i, d)

            def one(i=i, xq=xq, zq=zq):
                fn(i, xq, zq)

            pl.when(needed(yl_from, xq, zq))(one)

    def ly_copy(side, xq, zq):
        if side == 2:
            there = (y + jnp.where(yl == 1, 3, 1)) % 4
            target = (y + jnp.where(yl == 1, 1, 3)) % 4
            ref = lall.at[there % 2, there // 2, xq, zq]
            device = (z, target // 2, target % 2, x, h)
        else:
            ref = lall.at[yl, yh, xq, zq]
            device = yp if side == 0 else ym
        return copy(ref, ref, S_LY + 16 * side + xq * 4 + zq, device)

    def ly_wait(side, xq, zq):
        ref = lall.at[yl, yh, xq, zq]
        copy(ref, ref, S_LY + 16 * side + xq * 4 + zq, yp).wait_recv()

    def ly_start(d):
        @pl.when(mine_l)
        def _():
            def fn(i, xq, zq):
                ly_copy(0, xq, zq).start()
                ly_copy(1, xq, zq).start()

            l_each(d, yl, fn)

    def ly_forward(d):
        @pl.when(beside_l)
        def _():
            def fn(i, xq, zq):
                ly_wait(jnp.where(yl == 1, 0, 1), xq, zq)
                ly_copy(2, xq, zq).start()

            l_each(d, 1 - yl, fn)

    @pl.when(jnp.logical_and(mine_l, needed(yl, x, z)))
    def _():
        for j in range(1, 4):
            l1_copy(j).start()

    below_copy(me_r, 1, 2, zp).start()
    below_copy(me_r, 0, 2, zm).start()

    def source(step, half):
        late = jnp.logical_or(step == 3, step >= 5)
        down = jnp.logical_or(step == 1, step == 5)
        up = jnp.logical_or(step == 2, step == 6)
        dz = jnp.where(down, 3 - 2 * half, jnp.where(up, 1 + 2 * half, 0))
        dz = jnp.where(jnp.logical_or(step == 4, step == 7), 2, dz)
        return ((z + dz) % 4) * 2 + (yh + jnp.where(late, 1, 0)) % 2

    def pair_copy(s, share):
        where = rows_at(share * 4, 4)
        return copy(part.at[s % 4, 1 - h, where], pair.at[s, where], S_PAIR + 4 * s + share, partner)

    def add_pair(s, share):
        pair_copy(s, share).wait_recv()

        def add(i, carry):
            where = rows_at(share * 4 + i, 1)
            part[s % 4, h, where] += pair[s, where]
            return carry

        lax.fori_loop(0, 4, add, 0)

    def a_copy(s, side):
        far = (x + 2) % 4
        src = part.at[s % 4, h, rows_at(far * 4 + 2 * side, 2)]
        return copy(src, rec_a.at[s, side], S_A + 2 * s + side, xp if side == 0 else xm)

    def b_copy(s, side):
        near = (x + (1 if side == 0 else 3)) % 4
        src = part.at[s % 4, h, rows_at(near * 4, 4)]
        return copy(src, rec_b.at[s, side], S_B + 2 * s + side, xp if side == 0 else xm)

    def y_copy(s):
        return copy(xy.at[s, rows_at((1 - yl) * 2, 2)], rec_y.at[s], S_Y + s, ypair)

    def step_body(t, carry):
        @pl.when(t < 8)
        def _():
            load_m(2 * t).start()
            load_m(2 * t + 1).start()

        @pl.when(t == 2)
        def _():
            @pl.when(mine_l)
            def _():
                for j in range(1, 4):
                    l1_wait(j)

                def fn(i, xq, zq):
                    l2_copy(0, i).start()
                    l2_copy(1, i).start()

                l_each(0, yl, fn)

            ly_start(0)

        def second_halves():
            below_copy(source(3, 1), 1, 6, zp).start()
            below_copy(source(3, 0), 0, 6, zm).start()

        @pl.when(t == 4)
        def _():
            pl.when(h == 0)(second_halves)

            @pl.when(mine_l)
            def _():
                def from_down(i, xq, zq):
                    l2_copy(0, i).wait_recv()
                    if i % 2 == 0:
                        l2_forward(i).start()

                def from_up(i, xq, zq):
                    l2_copy(1, i).wait_recv()
                    if i % 2 == 1:
                        l2_forward(i).start()

                l_each(3, yl, from_down)
                l_each(1, yl, from_up)

            pl.when(h == 1)(second_halves)
            ly_start(1)
            ly_start(3)

        @pl.when(t == 5)
        def _():
            ly_forward(0)

        @pl.when(t == 6)
        def _():
            @pl.when(mine_l)
            def _():
                l_each(2, yl, lambda i, xq, zq: l2_forward(i).wait_recv())

            ly_start(2)
            ly_forward(1)

        @pl.when(t == 7)
        def _():
            ly_forward(3)

        @pl.when(t == 8)
        def _():
            ly_forward(2)

        @pl.when(jnp.logical_and(t > 0, t < 8))
        def _():
            for k in range(2):
                below_copy(source(t, k), k, t, zp).wait_recv()

        @pl.when(t == 1)
        def _():
            below_copy(source(1, 0), 0, 4, zp).start()
            below_copy(source(1, 1), 1, 4, zm).start()

        @pl.when(t == 3)
        def _():
            r = source(3, 0)
            below_copy(r, 0, 5, zp).start()
            below_copy(r, 1, 5, zm).start()

        @pl.when(t == 5)
        def _():
            below_copy(source(5, 0), 0, 7, zp).start()
            below_copy(source(5, 1), 1, 7, zm).start()

        @pl.when(t < 8)
        def _():
            for k in range(2):
                for q in range(7):
                    hi, lo = split(ball[source(t, k), k, q])
                    where = slice(k * 128, (k + 1) * 128)
                    bcat[where, q * 128:(q + 1) * 128] = hi
                    bcat[where, (7 + q) * 128:(8 + q) * 128] = hi
                    bcat[where, (14 + q) * 128:(15 + q) * 128] = lo

            def quarter(i, carry):
                share = (x + 2 + i) % 4
                for u in range(2):
                    where = rows_at(share * 4 + 2 * u, 2)
                    value = dot_t(rcat[where, 0:1792], bcat[:, 0:1792]) + dot_t(rcat[where, 0:896], bcat[:, 1792:2688])
                    part[t % 4, 0, where] = value[:, :128]
                    part[t % 4, 1, where] = value[:, 128:]

                @pl.when(jnp.logical_and(x * 2 + h == source(t, yl), share == 0))
                def _():
                    for k in range(2):
                        part[t % 4, yl, k * 256:k * 256 + 128] -= ublk[k]

                pair_copy(t, share).start()
                return carry

            lax.fori_loop(0, 4, quarter, 0)

            add_pair(t, (x + 2) % 4)
            a_copy(t, 0).start()
            a_copy(t, 1).start()

            for slot in range(2):
                load_m(2 * t + slot).wait()
                value = mstage[slot]
                sums[0, 0] += jnp.sum((value * value).reshape(128, 8, 128), axis=0)

        @pl.when(t == 0)
        def _():
            copy(yfwd.at[0], yfwd.at[0], S_FWD, yp).wait_recv()
            copy(yfwd.at[1], yfwd.at[1], S_FWD + 1, ym).wait_recv()
            back = (y + 3) % 4
            copy(yfwd.at[0], ball.at[z * 2 + back // 2, 0], S_BELOW + 6, yp).start()
            ahead = (y + 1) % 4
            copy(yfwd.at[1], ball.at[z * 2 + ahead // 2, 1], S_BELOW + 7, ym).start()

        @pl.when(jnp.logical_and(t >= 1, t < 9))
        def _():
            s = t - 1
            for side in range(2):
                near = (x + (1 if side == 0 else 3)) % 4
                add_pair(s, near)
                a_copy(s, side).wait_recv()
                where = rows_at(near * 4 + 2 * side, 2)
                part[s % 4, h, where] += rec_a[s, side]
                b_copy(s, side).start()
            add_pair(s, x)

        @pl.when(t >= 2)
        def _():
            s = t - 2
            b_copy(s, 0).wait_recv()
            b_copy(s, 1).wait_recv()

            def add(i, carry):
                where = rows_at(i, 1)
                xy[s, where] = part[s % 4, h, rows_at(x * 4 + i, 1)] + rec_b[s, 0, where] + rec_b[s, 1, where]
                return carry

            lax.fori_loop(0, 4, add, 0)
            y_copy(s).start()
            for share in range(4):
                pair_copy(s, share).wait_send()
            for side in range(2):
                a_copy(s, side).wait_send()
                b_copy(s, side).wait_send()

        return carry

    lax.fori_loop(0, 10, step_body, 0)

    def take_y(s, carry):
        y_copy(s).wait_recv()
        hi, lo = split(xy[s, rows_at(yl * 2, 2)] + rec_y[s])
        xs[0, s] = hi
        xs[1, s] = lo
        return carry

    def ly_last(yl_from, fn):
        for d in range(4):
            l_each(d, yl_from, fn)

    def product(i, first, last):
        for s in range(first, last):
            r = source(s, h)
            piece = lall[i // 4, r % 2, i % 4, r // 2]
            hi, lo = split(jnp.where(needed(i // 4, i % 4, r // 2), piece, 0.0))
            lsplit[0, s * 128:(s + 1) * 128] = hi
            lsplit[1, s * 128:(s + 1) * 128] = lo
        rows = slice(first * 128, last * 128)
        left = jnp.concatenate([xs[0, s] for s in range(first, last)], axis=1)
        rest_of = jnp.concatenate([xs[1, s] for s in range(first, last)], axis=1)
        value = dot_n(left, lsplit[0, rows]) + dot_n(rest_of, lsplit[0, rows]) + dot_n(left, lsplit[1, rows])
        if first == 0:
            acc[i] = value
        else:
            acc[i] += value

    def first_part(i, carry):
        product(i, 0, 6)
        return carry

    lax.fori_loop(0, 6, take_y, 0)

    @pl.when(mine_l)
    def _():
        ly_last(yl, lambda i, xq, zq: ly_wait(2, xq, zq))

    @pl.when(beside_l)
    def _():
        ly_last(1 - yl, lambda i, xq, zq: ly_wait(jnp.where(yl == 1, 1, 0), xq, zq))

    lax.fori_loop(0, 4 + 4 * h, first_part, 0)
    lax.fori_loop(6, 8, take_y, 0)

    def out_copy(i):
        return copy(acc.at[i], acc_in.at[i], S_OUT + i, partner)

    def mirror_row(j, side, other):
        to_z = (z + j) % 4
        src = acc.at[4 * h + to_z, :, side * 128:(side + 1) * 128]
        if other and j == 0:
            return copy(src, mfwd.at[0], S_MF, ym)
        if other and j == 3:
            return copy(src, mfwd.at[1], S_MF + 1, ym)
        if other and j == 2:
            return copy(src, mfwd.at[2], S_MF + 2, zm)
        return copy(src, m1.at[me_r], S_M1 + 2 * j + other, (to_z, side, yl, x, h))

    ahead = ((y + 1) % 4) // 2

    def mirror_row_on(slot):
        if slot == 0:
            return copy(mfwd.at[0], m1.at[z * 2 + ahead], S_M1 + 1, ym)
        if slot == 1:
            return copy(mfwd.at[1], m1.at[z * 2 + ahead], S_M1 + 7, (zm[0], *ym[1:]))
        return copy(mfwd.at[2], m1.at[((z + 1) % 4) * 2 + yh], S_M1 + 5, dev(dz=3, dyh=1))

    def mirror_row_in(j, other):
        from_z, from_y = (z + 4 - j) % 4, (yh + other) % 2
        ref = m1.at[from_z * 2 + from_y]
        return copy(ref, ref, S_M1 + 2 * j + other, zp)

    @pl.when(h == 1)
    def _():
        def early(j, carry):
            i = (z + 2 + j) % 4
            product(i, 6, 8)
            out_copy(i).start()
            return carry

        lax.fori_loop(0, 4, early, 0)

    def late(j0, carry):
        j = (j0 + 2) % 4
        i = (z + j) % 4
        product(4 * h + i, 6, 8)

        @pl.when(h == 0)
        def _():
            out_copy(i).wait_recv()
            acc[i] += acc_in[i]

        for side in range(2):
            for step in range(4):
                for other in range(2):
                    @pl.when(jnp.logical_and(j == step, (yh + other) % 2 == side))
                    def _():
                        if step == 0 and other == 0:
                            m1[me_r] = acc[4 * h + z, :, side * 128:(side + 1) * 128]
                        else:
                            mirror_row(step, side, other).start()

        value = acc[4 * h + i]
        value = value * value
        sums[0, 1] += jnp.sum((value[:, :128] + value[:, 128:]).reshape(32, 8, 128), axis=0)
        return carry

    lax.fori_loop(0, 4, late, 0)

    def sum_copies(phase):
        if phase == 0:
            devices = [dev(dx=j // 2, dh=j % 2) for j in range(1, 8)]
        else:
            devices = [dev_zy(j // 4, j % 4) for j in range(1, 16)]
        return [
            copy(sums.at[phase], sums_in.at[7 * phase + j], S_SUM + 7 * phase + j, device)
            for j, device in enumerate(devices)
        ]

    def take_sum(phase):
        copies = sum_copies(phase)
        for c in copies:
            c.wait_recv()
        total = sums[phase]
        for j in range(len(copies)):
            total += sums_in[7 * phase + j]
        return total

    for c in sum_copies(0):
        c.start()

    def mirror_col(to_x, to_h):
        index = S_M2 + 2 * ((to_x + 4 - x) % 4) + (to_h + h) % 2
        return copy(m1.at[to_x * 2 + to_h], m2.at[h, x], index, (z, yh, yl, to_x, to_h))

    def mirror_col_in(j):
        from_x, from_h = (x + 4 - j // 2) % 4, (h + j % 2) % 2
        ref = m2.at[from_h, from_x]
        return copy(ref, ref, S_M2 + j, xp)

    def send_on(slot):
        copy(mfwd.at[slot], mfwd.at[slot], S_MF + slot, zp).wait_recv()
        mirror_row_on(slot).start()

    def spread(j):
        from_z, from_y = (z + 4 - j // 2) % 4, (yh + j % 2) % 2
        if j > 0:
            mirror_row_in(j // 2, j % 2).wait_recv()
        here = jnp.logical_and(from_z == x, from_y == h)

        @pl.when(here)
        def _():
            m2[h, x] = m1[x * 2 + h]

        around = jnp.logical_and(from_z == (x + 2) % 4, j % 2 == 0)

        @pl.when(around)
        def _():
            copy(m1.at[from_z * 2 + from_y], mfwd.at[3], S_MF + 3, xm).start()

        @pl.when(jnp.logical_not(jnp.logical_or(here, around)))
        def _():
            mirror_col(from_z, from_y).start()

    spread(0)
    send_on(2)
    sums[1] = take_sum(0)
    for c in sum_copies(1):
        c.start()
    spread(6)
    send_on(1)
    send_on(0)
    spread(4)
    spread(2)
    copy(mfwd.at[3], mfwd.at[3], S_MF + 3, xm).wait_recv()
    copy(mfwd.at[3], m2.at[h, (x + 1) % 4], S_M2 + 4 + jnp.where(yh == h, 0, 1), (z, yh, yl, (x + 3) % 4, yh)).start()
    for j in (3, 5, 7, 1):
        spread(j)

    load_top.wait()
    total = take_sum(1)
    ratio = jnp.sum(total[1], axis=(0, 1), keepdims=True) / jnp.sum(total[0], axis=(0, 1), keepdims=True)
    balance = jnp.sqrt(jnp.sqrt(ratio))
    half = 0.5 * balance
    inverse = -0.5 / balance

    def finish(j0, carry):
        j = jnp.where(j0 < 4, j0, jnp.where(j0 < 6, j0 + 2, j0 - 2))

        @pl.when(j > 0)
        def _():
            mirror_col_in(j).wait_recv()

        k, xf = (h + j % 2) % 2, (x + 4 - j // 2) % 4
        for m in range(2):
            block = m2[k, xf, m * 128:(m + 1) * 128]
            where = pl.ds(2 * xf + m, 128, stride=8)
            out[k, where, :] = half * top[k, where, :] + inverse * block.T
        return carry

    lax.fori_loop(0, 8, finish, 0)

    for step in range(1, 8):
        for side in range(2):
            below_copy(me_r, side, step, zp).wait_send()
    for side in range(2):
        copy(ball.at[me_r, side], yfwd.at[side], S_FWD + side, yp).wait_send()
    swap_l.wait_send()

    @pl.when(mine_l)
    def _():
        @pl.when(needed(yl, x, z))
        def _():
            for j in range(1, 4):
                l1_copy(j).wait_send()

        def l2_sent(i, xq, zq):
            l2_copy(0, i).wait_send()
            l2_copy(1, i).wait_send()

        l_each(0, yl, l2_sent)
        l_each(3, yl, lambda i, xq, zq: l2_forward(i).wait_send() if i % 2 == 0 else None)
        l_each(1, yl, lambda i, xq, zq: l2_forward(i).wait_send() if i % 2 == 1 else None)

        def ly_sent(i, xq, zq):
            ly_copy(0, xq, zq).wait_send()
            ly_copy(1, xq, zq).wait_send()

        ly_last(yl, ly_sent)

    @pl.when(beside_l)
    def _():
        ly_last(1 - yl, lambda i, xq, zq: ly_copy(2, xq, zq).wait_send())

    def last_y(s, carry):
        y_copy(s).wait_send()
        return carry

    lax.fori_loop(0, 8, last_y, 0)

    @pl.when(h == 1)
    def _():
        for i in range(4):
            out_copy(i).wait_send()

    def last_mirror(j, carry):
        copy(m1.at[0], m1.at[0], S_M1 + j, zp).wait_send()
        copy(m1.at[0], m1.at[0], S_M2 + j, xp).wait_send()
        return carry

    lax.fori_loop(1, 8, last_mirror, 0)
    for slot in range(4):
        copy(mfwd.at[slot], mfwd.at[slot], S_MF + slot, zp).wait_send()
    for phase in range(2):
        for c in sum_copies(phase):
            c.wait_send()


def per_device(matrix, inverse_rest, upper_block, lower_below, lower_inverse):
    vmem = pltpu.VMEM
    dma = pltpu.SemaphoreType.DMA
    result = pl.pallas_call(
        kernel,
        out_shape=pltpu.VMEM((2, 1024, 128), F32),
        in_specs=[pl.BlockSpec(memory_space=ANY)] * 5,
        out_specs=pl.BlockSpec(memory_space=pltpu.VMEM),
        scratch_shapes=[
            vmem((8, 2, 7, 128, 128), F32),
            vmem((2, 7, 128, 128), F32),
            vmem((2048, 1792), BF16),
            vmem((256, 2688), BF16),
            vmem((4, 2, 2048, 128), F32),
            vmem((8, 2048, 128), F32),
            vmem((8, 2, 256, 128), F32),
            vmem((8, 2, 512, 128), F32),
            vmem((8, 256, 128), F32),
            vmem((8, 512, 128), F32),
            vmem((2, 8, 256, 128), BF16),
            vmem((2, 2, 4, 4, 128, 256), F32),
            vmem((2, 1024, 256), BF16),
            vmem((8, 256, 256), F32),
            vmem((4, 256, 256), F32),
            vmem((8, 256, 128), F32),
            vmem((2, 4, 256, 128), F32),
            vmem((4, 256, 128), F32),
            vmem((2, 1024, 128), F32),
            vmem((2, 1024, 128), F32),
            vmem((2, 128, 128), F32),
            vmem((2, 128, 128), F32),
            vmem((2, 2, 8, 128), F32),
            vmem((22, 2, 8, 128), F32),
            dma((5,)),
            dma((16,)),
            dma((2,)),
            dma((N_SEM,)),
            dma((N_SEM,)),
        ],
        compiler_params=pltpu.CompilerParams(
            collective_id=0, has_side_effects=True, vmem_limit_bytes=64500000
        ),
    )(
        matrix.reshape(16, 1024, 128),
        inverse_rest.transpose(0, 2, 1, 3).reshape(16, 896, 128),
        upper_block.reshape(2, 128, 128),
        lower_below.transpose(0, 2, 1, 3),
        lower_inverse,
    )
    return result.reshape(2, 128, 8, 128)


def solution(mesh):
    split_mesh = Mesh(mesh.devices.reshape(4, 2, 2, 4, 2), ("row_0", "row_1", "col_0", "col_1", "col_2"))
    return jax.shard_map(
        per_device,
        mesh=split_mesh,
        in_specs=(
            P(None, ROW, None, COL),
            P(None, ROW, None, COL),
            P(None, ROW, None, COL),
            P(None, ROW, None, COL),
            P(None, ROW, COL),
        ),
        out_specs=P(None, ROW, None, COL),
        check_vma=False,
    )
```
